256 devices in a mesh: dp: 16 (over z, core), feat: 16 (over x, y).
Axes of the slice: x: 4, y: 4, z: 8, core: 2. Of those that a mesh axis runs over, the one named last changes fastest.
Arguments:
- points: bfloat16 [4096, 256], P('dp'), may hold values from -6 to 6
- freqs: bfloat16 [256, 8192], P(None, 'feat'), may hold values from -0.375 to 0.375
- phase: float32 [8192], P('feat'), may hold values from -3.140625 to 3.140625
- ridge: float32 [8192], P('feat'), may hold values from 0.05 to 0.5
- targets: bfloat16 [8, 4096], P(None, 'dp'), may hold values from -6 to 6
Outputs:
- gram: float32 [8192, 8192], P('feat', 'dp')
- projected: float32 [8, 8192], P(None, 'feat')
- factors: float32 [8192, 1024], P('feat')
The draws below stay inside these ranges and needn't reach their ends.
All inputs are finite; a program needn't handle non-finite values.
Results may differ from the reference program's by a relative error of at most 0.003.
Values may be sent and summed in bfloat16 or wider, within the bound.
A program may use at most 128 MiB of HBM per device.

```python
import math
import jax
import jax.numpy as jnp
from jax import lax

DIN = 256
OUTS = 8
FB = 1024
F = 8192
ROWS = 4096


def steps_of(rng, shape, pieces, smallest, top_value):
    def one(position, blocks):
        steps = jax.random.uniform(jax.random.fold_in(jax.random.fold_in(rng, 6), position), (blocks,), jnp.float32, smallest / len(pieces), top_value / len(pieces))
        return jnp.repeat(jnp.exp(steps), shape[position] // blocks).reshape((-1,) + (1,) * (len(shape) - position - 1))

    gain = one(*pieces[0])
    for cut in pieces[1:]:
        gain = gain * one(*cut)
    return gain


def gaussian(own_key, extent, spread, limit, cuts=(), held_as=jnp.bfloat16):
    array = jax.random.normal(own_key, extent, jnp.float32) * spread
    if len(cuts) > 0:
        array = steps_of(own_key, extent, cuts, -0.22, 0.18) * array
    return jnp.clip(array, min=-limit, max=limit).astype(held_as)


def setup_inputs(seed: int = 0) -> dict:
    keys = jax.random.split(jax.random.key(seed), 6)
    points = gaussian(keys[0], (ROWS, DIN), 1.0, 6.0, ((0, 16),))
    freqs = gaussian(keys[1], (DIN, F), DIN ** -0.5, 0.375, ((1, 16),))
    phase = jnp.clip(jax.random.uniform(keys[2], (F,), jnp.float32, -3.140625, 3.140625), -3.140625, 3.140625)
    ridge = jnp.clip(jnp.exp(math.log(0.5) - 2.3025851 * jax.random.uniform(keys[3], (F,), jnp.float32) ** steps_of(keys[3], (F,), ((0, 16),), -0.2, 0.2)), 0.05, 0.5)
    targets = gaussian(keys[4], (OUTS, ROWS), 1.0, 6.0, ((1, 16),))
    return {"points": points, "freqs": freqs, "phase": phase, "ridge": ridge, "targets": targets}


def reference(points, freqs, phase, ridge, targets):
    scale = math.sqrt(2.0 / ROWS)
    angle = jnp.dot(points.astype(jnp.float32), freqs.astype(jnp.float32), preferred_element_type=jnp.float32) + phase
    phi = (scale * jnp.cos(angle)).astype(jnp.bfloat16)
    phi_wide = phi.astype(jnp.float32)
    gram = jnp.dot(phi_wide.T, phi_wide, precision=lax.Precision.HIGHEST) + jnp.diag(ridge)
    projected = jnp.dot(targets.astype(jnp.float32), phi_wide, precision=lax.Precision.HIGHEST)
    blocks = jnp.stack([gram[block_number * FB:(block_number + 1) * FB, block_number * FB:(block_number + 1) * FB] for block_number in range(OUTS)])
    factors = jnp.linalg.cholesky(blocks).reshape(F, FB)
    return (gram, projected, factors)
```

```python
import functools
import math

import jax
import jax.numpy as jnp
from jax import lax
from jax.experimental import pallas as pl
from jax.experimental.pallas import tpu as pltpu
from jax.sharding import PartitionSpec as P

FB = 1024
NB = 128
HI = lax.Precision.HIGHEST
TURN = 1.0 / (2.0 * math.pi)
C1, C3, C5, C7 = -6.283164044054801, 41.33714233314145, -81.34076747300007, 70.99341851060123


def cos_turns(turns, scale):
    r = turns - jnp.round(turns)
    u = jnp.abs(r) - 0.25
    w = u * u
    poly = ((C7 * scale * w + C5 * scale) * w + C3 * scale) * w + C1 * scale
    return poly * u


def tdot(left, right, precision=None):
    return lax.dot_general(
        left, right, (((0,), (0,)), ((), ())), precision=precision, preferred_element_type=jnp.float32
    )


def row_of(x, r):
    return jnp.broadcast_to(x[r:r + 1, :], x.shape)


def lane_of(x, c):
    return jnp.broadcast_to(x[:, c:c + 1], x.shape)


def leaf(blocks):
    n = NB // 8
    sub = lax.broadcasted_iota(jnp.int32, (8, NB), 0)
    lane = lax.broadcasted_iota(jnp.int32, (8, NB), 1)
    a = list(blocks)
    e = [jnp.where(lane == sub + 8 * m, 1.0, 0.0).astype(jnp.float32) for m in range(n)]
    outs = []
    for k in range(n):
        pa, pe = a[k], e[k]
        v = [lane_of(pa, 8 * k + c) for c in range(8)]
        cols = {m: [lane_of(a[m], 8 * k + c) for c in range(8)] for m in range(k + 1, n)}
        nxt = k + 1 < n
        if nxt:
            na, ne = a[k + 1], e[k + 1]
            nv = list(cols[k + 1])
        rs = jnp.zeros((8, NB), jnp.float32)
        dv = jnp.zeros((8, NB), jnp.float32)
        for r in range(8):
            d = row_of(v[r], r)
            inv = 1.0 / d
            rs = jnp.where(sub == r, lax.rsqrt(d), rs)
            dv = jnp.where(sub == r, inv, dv)
            l = jnp.where(sub > r, v[r] * inv, 0.0)
            ba, be = row_of(pa, r), row_of(pe, r)
            if nxt:
                l1 = nv[r] * inv
                na = na - l1 * ba
                ne = ne - l1 * be
            pa = pa - l * ba
            pe = pe - l * be
            for c in range(r + 1, 8):
                b = row_of(v[c], r)
                v[c] = v[c] - l * b
                if nxt:
                    nv[c] = nv[c] - l1 * b
        outs.append((pa * rs, pe * rs))
        if nxt:
            a[k + 1], e[k + 1] = na, ne
        if k + 2 < n:
            qa, qe = pa * dv, pe * dv
            for r in range(7, 0, -1):
                mult = jnp.where(sub < r, v[r] * dv, 0.0)
                qa = qa - mult * row_of(qa, r)
                qe = qe - mult * row_of(qe, r)
            ra = [row_of(qa, r) for r in range(8)]
            re = [row_of(qe, r) for r in range(8)]
            for m in range(k + 2, n):
                ma = [cols[m][r] * ra[r] for r in range(8)]
                me = [cols[m][r] * re[r] for r in range(8)]
                while len(ma) > 1:
                    ma = [ma[i] + ma[i + 1] for i in range(0, len(ma), 2)]
                    me = [me[i] + me[i + 1] for i in range(0, len(me), 2)]
                a[m] = a[m] - ma[0]
                e[m] = e[m] - me[0]
    return outs


def kernel(scale, feat_axis, data_axis, pts, tgt, fw, fd, phw, phd, rdg, gram, proj, fac, wphi, cphi, slab, ue, own_phi):
    rows = pts.shape[0]
    half = fd.shape[1]
    feat = lax.axis_index(feat_axis)
    data = lax.axis_index(data_axis)
    odd = lax.rem(feat, FB // half)
    own = pl.multiple_of(odd * half, half)

    def chunk(i, _):
        at = pl.ds(pl.multiple_of(i * 256, 256), 256)
        p = pts[at, :]
        for src, ph, dst, width in ((fw, phw, wphi, FB), (fd, phd, cphi, half)):
            for j in range(0, width, 256):
                ang = jnp.dot(p, src[:, j:j + 256], preferred_element_type=jnp.float32)
                dst[at, j:j + 256] = cos_turns(ang * TURN + ph[:, j:j + 256], scale).astype(jnp.bfloat16)
        return 0

    lax.fori_loop(0, rows // 256, chunk, 0)

    own_phi[...] = wphi[:, pl.ds(own, half)]
    proj[...] = jnp.dot(tgt[...], own_phi[...], preferred_element_type=jnp.float32)
    gram[...] = tdot(own_phi[...], cphi[...])

    def eye_add(ref, row0, rvec):
        n = rvec.shape[1]
        for i in range(0, n, NB):
            eye = lax.broadcasted_iota(jnp.int32, (NB, NB), 0) == lax.broadcasted_iota(jnp.int32, (NB, NB), 1)
            ref[row0 + i:row0 + i + NB, i:i + NB] += jnp.where(eye, rvec[:, i:i + NB], 0.0)

    @pl.when(feat == data)
    def _():
        eye_add(gram, 0, rdg[:, pl.ds(own, half)])

    slab[0:512, :] = tdot(wphi[:, 0:512], wphi[...])
    slab[512:1024, 512:1024] = tdot(wphi[:, 512:1024], wphi[:, 512:1024])
    eye_add(slab, 0, rdg[...])

    nblk = FB // NB

    def step(k, _):
        at = pl.multiple_of(k * NB, NB)
        blocks = [slab[pl.ds(pl.multiple_of(at + 8 * m, 8), 8), pl.ds(at, NB)] for m in range(NB // 8)]
        sub = lax.broadcasted_iota(jnp.int32, (8, NB), 0)
        lane = lax.broadcasted_iota(jnp.int32, (8, NB), 1)
        for m, (u, x) in enumerate(leaf(blocks)):
            slab[pl.ds(pl.multiple_of(at + 8 * m, 8), 8), pl.ds(at, NB)] = jnp.where(lane >= sub + 8 * m, u, 0.0)
            ue[8 * m:8 * m + 8, :] = x
        for kk in range(nblk - 1):
            @pl.when(k == kk)
            def _():
                lo, mid = kk * NB, (kk + 1) * NB
                u12 = jnp.dot(ue[...], slab[lo:mid, mid:], precision=HI, preferred_element_type=jnp.float32)
                slab[lo:mid, mid:] = u12
                for i in range(mid, FB, 256):
                    w = min(256, FB - i)
                    slab[i:i + w, i:] -= tdot(u12[:, i - mid:i - mid + w], u12[:, i - mid:], HI)
        return 0

    lax.fori_loop(0, nblk, step, 0)

    for b in range(half // NB):
        for j in range(nblk):
            piece = jnp.transpose(slab[j * NB:(j + 1) * NB, pl.ds(pl.multiple_of(own + b * NB, NB), NB)])
            keep = j * NB <= own + b * NB
            fac[b * NB:(b + 1) * NB, j * NB:(j + 1) * NB] = jnp.where(keep, piece, 0.0)


def local(scale, pts, tgt, fw, fd, phw, phd, rdg, interpret=False):
    rows, half = pts.shape[0], fd.shape[1]
    f32 = jnp.float32
    return pl.pallas_call(
        functools.partial(kernel, scale, "feat", "dp"),
        out_shape=(
            jax.ShapeDtypeStruct((half, half), f32),
            jax.ShapeDtypeStruct((8, half), f32),
            jax.ShapeDtypeStruct((half, FB), f32),
        ),
        scratch_shapes=[
            pltpu.VMEM((rows, FB), jnp.bfloat16),
            pltpu.VMEM((rows, half), jnp.bfloat16),
            pltpu.VMEM((FB, FB), f32),
            pltpu.VMEM((NB, NB), f32),
            pltpu.VMEM((rows, half), jnp.bfloat16),
        ],
        compiler_params=pltpu.CompilerParams(vmem_limit_bytes=60 * 1024 * 1024),
        interpret=interpret,
    )(pts, tgt, fw, fd, phw, phd, rdg)


def shards(points, freqs, phase, ridge, targets):
    data_count = lax.axis_size("dp")
    feat_count = lax.axis_size("feat")
    feat = lax.axis_index("feat")
    rows = points.shape[0]
    half = freqs.shape[1]
    scale = math.sqrt(2.0 / (rows * data_count))
    pack = lax.all_gather(jnp.concatenate([points, targets], 0), "dp", axis=0)
    points_all = pack[:, :rows].reshape(rows * data_count, -1)
    targets_all = jnp.transpose(pack[:, rows:], (1, 0, 2)).reshape(targets.shape[0], -1)
    small = jnp.stack([phase * TURN, ridge])
    pair = [(i, i ^ 1) for i in range(feat_count)]
    swap = [(d * feat_count + f, f * feat_count + d) for d in range(data_count) for f in range(feat_count)]
    f_other, s_other = lax.ppermute(freqs, "feat", pair), lax.ppermute(small, "feat", pair)
    f_tile, s_tile = lax.ppermute(freqs, ("dp", "feat"), swap), lax.ppermute(small, ("dp", "feat"), swap)
    odd = lax.rem(feat, 2) == 1
    fw = jnp.where(odd, jnp.concatenate([f_other, freqs], 1), jnp.concatenate([freqs, f_other], 1))
    sw = jnp.where(odd, jnp.concatenate([s_other, small], 1), jnp.concatenate([small, s_other], 1))
    return local(scale, points_all, targets_all, fw, f_tile, sw[0:1], s_tile[0:1], sw[1:2])


def solution(mesh):
    in_specs = (P("dp", None), P(None, "feat"), P("feat"), P("feat"), P(None, "dp"))
    out_specs = (P("feat", "dp"), P(None, "feat"), P("feat", None))
    return jax.shard_map(shards, mesh=mesh, in_specs=in_specs, out_specs=out_specs, check_vma=False)
```

```python
import functools
import math

import jax
import jax.numpy as jnp
from jax import lax
from jax.experimental import pallas as pl
from jax.experimental.pallas import tpu as pltpu
from jax.sharding import PartitionSpec as P

FB = 1024
NB = 128
XS = 4
YS = 4
ZS = 8
HI = lax.Precision.HIGHEST
MESH = pl.DeviceIdType.MESH
TURN = 1.0 / (2.0 * math.pi)
C1, C3, C5, C7 = -6.283164044054801, 41.33714233314145, -81.34076747300007, 70.99341851060123


def exchange(pack, freqs, small, points, other_f, other_s, tile_f, tile_s,
             up_send, up_recv, dn_send, dn_recv, mate_send, mate_recv,
             pair_send, pair_recv, tree_recv, row_send, col_send, local_sem):
    data, feat = lax.axis_index("dp"), lax.axis_index("feat")
    z, core = data // 2, data % 2
    x, y = feat // YS, feat % YS
    first = 128

    def at(zz, cc):
        return {"dp": zz * 2 + cc, "feat": feat}

    def near(xx, yy):
        return {"dp": data, "feat": xx * YS + yy}

    up, dn = (z + 1) % ZS, (z + ZS - 1) % ZS
    barrier = pltpu.get_barrier_semaphore()
    peers = [at(up, core), at(dn, core), at(z, 1 - core)]
    peers += [near((x + i) % XS, y) for i in range(1, XS)] + [near(x, (y + i) % YS) for i in range(1, YS)]
    for peer in peers:
        pl.semaphore_signal(barrier, inc=1, device_id=peer, device_id_type=MESH)
    pl.semaphore_wait(barrier, len(peers))

    pieces = (pl.ds(0, first), pl.ds(first, pack.shape[0] - first))

    def remote(src, dst, ssem, rsem, where):
        return pltpu.make_async_remote_copy(
            src_ref=src, dst_ref=dst, send_sem=ssem, recv_sem=rsem, device_id=where, device_id_type=MESH)

    sends = []

    def go(copy):
        copy.start()
        sends.append(copy)
        return copy

    def slot(zz):
        return ((zz + 2 * ZS) % ZS) * 2 + core

    def ring(step, p, upward):
        zz = z - step if upward else z + step
        src = pack.at[pieces[p]] if step == 0 else points.at[slot(zz), pieces[p]]
        dst = points.at[slot(zz), pieces[p]]
        if upward:
            return remote(src, dst, up_send.at[step, p], up_recv.at[step, p], at(up, core))
        return remote(src, dst, dn_send.at[step, p], dn_recv.at[step, p], at(dn, core))

    def mate(i, p, zz, own=False):
        src = pack.at[pieces[p]] if own else points.at[slot(zz), pieces[p]]
        return remote(src, points.at[slot(zz), pieces[p]], mate_send.at[i, p], mate_recv.at[i, p], at(z, 1 - core))

    for p in range(2):
        go(ring(0, p, True))
        go(ring(0, p, False))
    pair_y = y + 1 - 2 * (y % 2)
    pair_copies = [
        remote(small, other_s, pair_send.at[0], pair_recv.at[0], near(x, pair_y)),
        remote(freqs, other_f, pair_send.at[1], pair_recv.at[1], near(x, pair_y)),
    ]
    for copy in pair_copies:
        go(copy)
    keep = pltpu.make_async_copy(pack, points.at[slot(z)], local_sem.at[0])
    keep.start()
    for p in range(2):
        go(mate(0, p, z, own=True))

    rx, ry = data // YS, data % YS
    parts = [(small, tile_s, None), (freqs, tile_f, pl.ds(0, 128)), (freqs, tile_f, pl.ds(128, 128))]

    def part(ref, cut):
        return ref if cut is None else ref.at[cut]

    def to_row(n, i):
        src, dst, cut = parts[n]
        return remote(part(src, cut), part(dst, cut), row_send.at[n, i], tree_recv.at[n], near((x + i + 1) % XS, y))

    def to_col(n, i, own):
        src, dst, cut = parts[n]
        return remote(part(src if own else dst, cut), part(dst, cut), col_send.at[n, i], tree_recv.at[n],
                      near(x, (y + i + 1) % YS))

    root = jnp.logical_and(x == rx, y == ry)
    mid = jnp.logical_and(x != rx, y == ry)

    @pl.when(root)
    def _():
        for n in range(3):
            for i in range(XS - 1):
                to_row(n, i).start()
            for i in range(YS - 1):
                to_col(n, i, True).start()
        a = pltpu.make_async_copy(freqs, tile_f, local_sem.at[1])
        b = pltpu.make_async_copy(small, tile_s, local_sem.at[2])
        a.start()
        b.start()
        a.wait()
        b.wait()

    def pass_on(n):
        @pl.when(mid)
        def _():
            to_row(n, 0).wait_recv()
            for i in range(YS - 1):
                to_col(n, i, False).start()

    for step in range(1, 5):
        todo = [(0, True), (0, False), (1, True), (1, False)] if step < 4 else [(0, True), (1, False)]
        for p, upward in todo:
            ring(step - 1, p, upward).wait_recv()
            if step < 3 or (step == 3 and p == (0 if upward else 1)):
                go(ring(step, p, upward))
            go(mate(2 * step - 1 + (0 if upward or step == 4 else 1), p, z - step if upward else z + step))
        if step == 1:
            pass_on(0)
            pass_on(1)
        if step == 2:
            pass_on(2)

    @pl.when(y != ry)
    def _():
        for n in range(3):
            to_col(n, 0, False).wait_recv()

    for i in range(8):
        for p in range(2):
            mate(i, p, z).wait_recv()
    for copy in pair_copies:
        copy.wait_recv()
    keep.wait()

    @pl.when(root)
    def _():
        for n in range(3):
            for i in range(XS - 1):
                to_row(n, i).wait_send()

    @pl.when(y == ry)
    def _():
        for n in range(3):
            for i in range(YS - 1):
                to_col(n, i, False).wait_send()

    for copy in sends:
        copy.wait_send()


def gather(pack, freqs, small):
    dma = pltpu.SemaphoreType.DMA
    vmem = pl.BlockSpec(memory_space=pltpu.VMEM)
    shape = jax.ShapeDtypeStruct
    return pl.pallas_call(
        exchange,
        out_shape=(
            shape((2 * ZS,) + pack.shape, pack.dtype),
            shape(freqs.shape, freqs.dtype),
            shape(small.shape, small.dtype),
            shape(freqs.shape, freqs.dtype),
            shape(small.shape, small.dtype),
        ),
        in_specs=[vmem] * 3,
        out_specs=(vmem,) * 5,
        scratch_shapes=[
            dma((4, 2)), dma((4, 2)), dma((4, 2)), dma((4, 2)), dma((8, 2)), dma((8, 2)),
            dma((2,)), dma((2,)), dma((3,)), dma((3, 3)), dma((3, 3)), dma((3,)),
        ],
        compiler_params=pltpu.CompilerParams(collective_id=0, has_side_effects=True),
    )(pack, freqs, small)


def cos_turns(turns, scale):
    r = turns - jnp.round(turns)
    u = jnp.abs(r) - 0.25
    w = u * u
    poly = ((C7 * scale * w + C5 * scale) * w + C3 * scale) * w + C1 * scale
    return poly * u


def tdot(left, right, precision=None):
    return lax.dot_general(
        left, right, (((0,), (0,)), ((), ())), precision=precision, preferred_element_type=jnp.float32
    )


def row_of(x, r):
    return jnp.broadcast_to(x[r:r + 1, :], x.shape)


def lane_of(x, c):
    return jnp.broadcast_to(x[:, c:c + 1], x.shape)


def leaf(blocks):
    n = NB // 8
    sub = lax.broadcasted_iota(jnp.int32, (8, NB), 0)
    lane = lax.broadcasted_iota(jnp.int32, (8, NB), 1)
    a = list(blocks)
    e = [jnp.where(lane == sub + 8 * m, 1.0, 0.0).astype(jnp.float32) for m in range(n)]
    outs = []
    for k in range(n):
        pa, pe = a[k], e[k]
        v = [lane_of(pa, 8 * k + c) for c in range(8)]
        cols = {m: [lane_of(a[m], 8 * k + c) for c in range(8)] for m in range(k + 1, n)}
        nxt = k + 1 < n
        if nxt:
            na, ne = a[k + 1], e[k + 1]
            nv = list(cols[k + 1])
        rs = jnp.zeros((8, NB), jnp.float32)
        dv = jnp.zeros((8, NB), jnp.float32)
        for r in range(8):
            d = row_of(v[r], r)
            inv = 1.0 / d
            rs = jnp.where(sub == r, lax.rsqrt(d), rs)
            dv = jnp.where(sub == r, inv, dv)
            l = jnp.where(sub > r, v[r] * inv, 0.0)
            ba, be = row_of(pa, r), row_of(pe, r)
            if nxt:
                l1 = nv[r] * inv
                na = na - l1 * ba
                ne = ne - l1 * be
            pa = pa - l * ba
            pe = pe - l * be
            for c in range(r + 1, 8):
                b = row_of(v[c], r)
                v[c] = v[c] - l * b
                if nxt:
                    nv[c] = nv[c] - l1 * b
        outs.append((pa * rs, pe * rs))
        if nxt:
            a[k + 1], e[k + 1] = na, ne
        if k + 2 < n:
            qa, qe = pa * dv, pe * dv
            for r in range(7, 0, -1):
                mult = jnp.where(sub < r, v[r] * dv, 0.0)
                qa = qa - mult * row_of(qa, r)
                qe = qe - mult * row_of(qe, r)
            ra = [row_of(qa, r) for r in range(8)]
            re = [row_of(qe, r) for r in range(8)]
            for m in range(k + 2, n):
                ma = [cols[m][r] * ra[r] for r in range(8)]
                me = [cols[m][r] * re[r] for r in range(8)]
                while len(ma) > 1:
                    ma = [ma[i] + ma[i + 1] for i in range(0, len(ma), 2)]
                    me = [me[i] + me[i + 1] for i in range(0, len(me), 2)]
                a[m] = a[m] - ma[0]
                e[m] = e[m] - me[0]
    return outs


def kernel(scale, feat_axis, data_axis, pts, fo, fp, fd, so, sp, sd, gram, proj, fac, wphi, cphi, slab, ue, own_phi, tgt):
    count = pts.shape[0]
    half = fd.shape[1]
    block = 256
    feat = lax.axis_index(feat_axis)
    data = lax.axis_index(data_axis)
    odd = lax.rem(feat, FB // half)
    own = pl.multiple_of(odd * half, half)
    oth = pl.multiple_of((1 - odd) * half, half)

    def chunk(i, _):
        at = pl.ds(pl.multiple_of(i * block, block), block)
        p = pts[i, 0:block, :]
        for src, sm, dst, base in ((fo, so, wphi, own), (fp, sp, wphi, oth), (fd, sd, cphi, 0)):
            for j in range(0, half, 256):
                ang = jnp.dot(p, src[:, j:j + 256], preferred_element_type=jnp.float32)
                to = pl.ds(pl.multiple_of(base + j, 256), 256)
                dst[at, to] = cos_turns(ang * TURN + sm[0:1, j:j + 256] * TURN, scale).astype(jnp.bfloat16)
        return 0

    lax.fori_loop(0, count, chunk, 0)

    for i in range(count):
        tgt[:, i * block:(i + 1) * block] = pts[i, block:block + 8, :]
    own_phi[...] = wphi[:, pl.ds(own, half)]
    proj[...] = jnp.dot(tgt[...], own_phi[...], preferred_element_type=jnp.float32)
    gram[...] = tdot(own_phi[...], cphi[...])
    eye = lax.broadcasted_iota(jnp.int32, (NB, NB), 0) == lax.broadcasted_iota(jnp.int32, (NB, NB), 1)

    @pl.when(feat == data)
    def _():
        for i in range(0, half, NB):
            gram[i:i + NB, i:i + NB] += jnp.where(eye, so[1:2, i:i + NB], 0.0)

    slab[0:512, :] = tdot(wphi[:, 0:512], wphi[...])
    slab[512:1024, 512:1024] = tdot(wphi[:, 512:1024], wphi[:, 512:1024])
    for sm, base in ((so, own), (sp, oth)):
        for i in range(0, half, NB):
            to = pl.ds(pl.multiple_of(base + i, NB), NB)
            slab[to, to] += jnp.where(eye, sm[1:2, i:i + NB], 0.0)

    nblk = FB // NB

    def step(k, _):
        at = pl.multiple_of(k * NB, NB)
        blocks = [slab[pl.ds(pl.multiple_of(at + 8 * m, 8), 8), pl.ds(at, NB)] for m in range(NB // 8)]
        sub = lax.broadcasted_iota(jnp.int32, (8, NB), 0)
        lane = lax.broadcasted_iota(jnp.int32, (8, NB), 1)
        for m, (u, x) in enumerate(leaf(blocks)):
            slab[pl.ds(pl.multiple_of(at + 8 * m, 8), 8), pl.ds(at, NB)] = jnp.where(lane >= sub + 8 * m, u, 0.0)
            ue[8 * m:8 * m + 8, :] = x
        for kk in range(nblk - 1):
            @pl.when(k == kk)
            def _():
                lo, mid = kk * NB, (kk + 1) * NB
                u12 = jnp.dot(ue[...], slab[lo:mid, mid:], precision=HI, preferred_element_type=jnp.float32)
                slab[lo:mid, mid:] = u12
                for i in range(mid, FB, 256):
                    w = min(256, FB - i)
                    slab[i:i + w, i:] -= tdot(u12[:, i - mid:i - mid + w], u12[:, i - mid:], HI)
        return 0

    lax.fori_loop(0, nblk, step, 0)

    for b in range(half // NB):
        for j in range(nblk):
            piece = jnp.transpose(slab[j * NB:(j + 1) * NB, pl.ds(pl.multiple_of(own + b * NB, NB), NB)])
            keep = j * NB <= own + b * NB
            fac[b * NB:(b + 1) * NB, j * NB:(j + 1) * NB] = jnp.where(keep, piece, 0.0)


def local(scale, pts, fo, fp, fd, so, sp, sd):
    rows, half = pts.shape[0] * 256, fd.shape[1]
    f32 = jnp.float32
    return pl.pallas_call(
        functools.partial(kernel, scale, "feat", "dp"),
        out_shape=(
            jax.ShapeDtypeStruct((half, half), f32),
            jax.ShapeDtypeStruct((8, half), f32),
            jax.ShapeDtypeStruct((half, FB), f32),
        ),
        scratch_shapes=[
            pltpu.VMEM((rows, FB), jnp.bfloat16),
            pltpu.VMEM((rows, half), jnp.bfloat16),
            pltpu.VMEM((FB, FB), f32),
            pltpu.VMEM((NB, NB), f32),
            pltpu.VMEM((rows, half), jnp.bfloat16),
            pltpu.VMEM((8, rows), jnp.bfloat16),
        ],
        compiler_params=pltpu.CompilerParams(vmem_limit_bytes=48 * 1024 * 1024),
    )(pts, fo, fp, fd, so, sp, sd)


def shards(points, freqs, phase, ridge, targets):
    scale = math.sqrt(2.0 / (points.shape[0] * lax.axis_size("dp")))
    pack = jnp.pad(jnp.concatenate([points, targets], 0), ((0, 8), (0, 0)))
    small = jnp.stack([phase, ridge])
    pts, other_f, other_s, tile_f, tile_s = gather(pack, freqs, small)
    return local(scale, pts, freqs, other_f, tile_f, small, other_s, tile_s)


def solution(mesh):
    in_specs = (P("dp", None), P(None, "feat"), P("feat"), P("feat"), P(None, "dp"))
    out_specs = (P("feat", "dp"), P(None, "feat"), P("feat", None))
    return jax.shard_map(shards, mesh=mesh, in_specs=in_specs, out_specs=out_specs, check_vma=False)
```

```python
import functools
import math

import jax
import jax.numpy as jnp
from jax import lax
from jax.experimental import pallas as pl
from jax.experimental.pallas import tpu as pltpu
from jax.sharding import PartitionSpec as P

FB = 1024
NB = 128
XS = 4
YS = 4
ZS = 8
HI = lax.Precision.HIGHEST
MESH = pl.DeviceIdType.MESH
TURN = 1.0 / (2.0 * math.pi)
C1, C3, C5, C7 = -6.283164044054801, 41.33714233314145, -81.34076747300007, 70.99341851060123


def cos_turns(turns, scale):
    r = turns - jnp.round(turns)
    u = jnp.abs(r) - 0.25
    w = u * u
    poly = ((C7 * scale * w + C5 * scale) * w + C3 * scale) * w + C1 * scale
    return poly * u


def tdot(left, right, precision=None):
    return lax.dot_general(
        left, right, (((0,), (0,)), ((), ())), precision=precision, preferred_element_type=jnp.float32
    )


def row_of(x, r):
    return jnp.broadcast_to(x[r:r + 1, :], x.shape)


def lane_of(x, c):
    return jnp.broadcast_to(x[:, c:c + 1], x.shape)


def leaf(blocks, one):
    n = NB // 8
    sub = lax.broadcasted_iota(jnp.int32, (8, NB), 0)
    lane = lax.broadcasted_iota(jnp.int32, (8, NB), 1)
    a = list(blocks)
    e = [jnp.where(lane == sub + 8 * m, 1.0, 0.0).astype(jnp.float32) for m in range(n)]

    def cols(m, k):
        return [lane_of(a[m], 8 * k + c) for c in range(8)]

    outs = []
    v, n1 = [x * one for x in cols(0, 0)], [x * one for x in cols(1, 0)]
    for k in range(n):
        pa, pe = a[k], e[k]
        has1, has2 = k + 1 < n, k + 2 < n
        far = {m: cols(m, k) for m in range(k + 2, n)}
        if has1:
            vn = cols(k + 1, k + 1)
        if has2:
            n2 = list(far[k + 2])
        rs = jnp.zeros((8, NB), jnp.float32)
        dv = jnp.zeros((8, NB), jnp.float32)
        for r in range(8):
            d = row_of(v[r], r)
            inv = 1.0 / d
            rs = jnp.where(sub == r, lax.rsqrt(d), rs)
            dv = jnp.where(sub == r, inv, dv)
            l = jnp.where(sub > r, v[r] * inv, 0.0)
            b = {c: row_of(v[c], r) for c in range(r + 1, 8)}
            ba, be = row_of(pa, r), row_of(pe, r)
            for c in b:
                v[c] = v[c] - l * b[c]
            pa = pa - l * ba
            pe = pe - l * be
            if has1:
                l1 = n1[r] * inv
                w = [row_of(n1[r], c) for c in range(8)]
                for c in b:
                    n1[c] = n1[c] - l1 * b[c]
                for c in range(8):
                    vn[c] = vn[c] - l1 * w[c]
                a[k + 1] = a[k + 1] - l1 * ba
                e[k + 1] = e[k + 1] - l1 * be
            if has2:
                l2 = n2[r] * inv
                for c in b:
                    n2[c] = n2[c] - l2 * b[c]
                a[k + 2] = a[k + 2] - l2 * ba
                e[k + 2] = e[k + 2] - l2 * be
        outs.append((pa * rs, pe * rs))
        if k + 3 < n:
            qa, qe = pa * dv, pe * dv
            for r in range(7, 0, -1):
                mult = jnp.where(sub < r, v[r] * dv, 0.0)
                qa = qa - mult * row_of(qa, r)
                qe = qe - mult * row_of(qe, r)
            ra = [row_of(qa, r) for r in range(8)]
            re = [row_of(qe, r) for r in range(8)]
            for m in range(k + 3, n):
                ma = [far[m][r] * ra[r] for r in range(8)]
                me = [far[m][r] * re[r] for r in range(8)]
                while len(ma) > 1:
                    ma = [ma[i] + ma[i + 1] for i in range(0, len(ma), 2)]
                    me = [me[i] + me[i + 1] for i in range(0, len(me), 2)]
                a[m] = a[m] - ma[0]
                e[m] = e[m] - me[0]
        if has1:
            v = vn
            if has2:
                n1 = [x * one for x in cols(k + 2, k + 1)]
    return outs


def fused(scale, pack, freqs, small, slab, gram, proj,
          points, other_f, other_s, tile_f, tile_s, wphi, cphi, tgt, slab_in, gram_out, gram_in, proj_in,
          up_send, up_recv, dn_send, dn_recv, pair_send, pair_recv, tree_recv, row_send, col_send,
          tile_send, tile_recv, swap_send, swap_recv, local_sem):
    data, feat = lax.axis_index("dp"), lax.axis_index("feat")
    z, core = data // 2, data % 2
    x, y = feat // YS, feat % YS
    block, half = 256, freqs.shape[1]
    odd = feat % 2
    own = pl.multiple_of(odd * half, half)
    oth = pl.multiple_of((1 - odd) * half, half)

    def at(zz, cc):
        return {"dp": zz * 2 + cc, "feat": feat}

    def near(xx, yy):
        return {"dp": data, "feat": xx * YS + yy}

    up, dn, mate = at((z + 1) % ZS, core), at((z + ZS - 1) % ZS, core), at(z, 1 - core)
    barrier = pltpu.get_barrier_semaphore()
    peers = [up, dn, mate]
    peers += [near((x + i) % XS, y) for i in range(1, XS)] + [near(x, (y + i) % YS) for i in range(1, YS)]
    for peer in peers:
        pl.semaphore_signal(barrier, inc=1, device_id=peer, device_id_type=MESH)
    pl.semaphore_wait(barrier, len(peers))

    first = 128
    pieces = (pl.ds(0, first), pl.ds(first, pack.shape[0] - first))
    sends = []

    def remote(src, dst, ssem, rsem, where):
        return pltpu.make_async_remote_copy(
            src_ref=src, dst_ref=dst, send_sem=ssem, recv_sem=rsem, device_id=where, device_id_type=MESH)

    def go(copy):
        copy.start()
        sends.append(copy)
        return copy

    def arrival(step, upward):
        return 7 if step == 4 else 2 * step - (1 if upward else 0)

    def ring(step, p, upward):
        src = pack if step == 0 else points.at[arrival(step, upward)]
        dst = points.at[arrival(step + 1, upward)]
        ssem, rsem, where = (up_send, up_recv, up) if upward else (dn_send, dn_recv, dn)
        return remote(src.at[pieces[p]], dst.at[pieces[p]], ssem.at[step, p], rsem.at[step, p], where)

    def ring_step(step):
        todo = [(0, True), (0, False), (1, True), (1, False)] if step < 4 else [(0, True), (1, False)]
        for p, upward in todo:
            ring(step - 1, p, upward).wait_recv()
            if step < 3 or (step == 3 and p == (0 if upward else 1)):
                go(ring(step, p, upward))

    for p in range(2):
        go(ring(0, p, True))
        go(ring(0, p, False))
    pair = near(x, y + 1 - 2 * (y % 2))
    pair_copies = [
        go(remote(small, other_s, pair_send.at[0], pair_recv.at[0], pair)),
        go(remote(freqs, other_f, pair_send.at[1], pair_recv.at[1], pair)),
    ]

    rx, ry = data // YS, data % YS
    parts = [(small, tile_s.at[0], None), (freqs, tile_f.at[0], pl.ds(0, 128)), (freqs, tile_f.at[0], pl.ds(128, 128))]

    def part(ref, cut):
        return ref if cut is None else ref.at[cut]

    def to_row(n, i):
        src, dst, cut = parts[n]
        return remote(part(src, cut), part(dst, cut), row_send.at[n, i], tree_recv.at[n], near((x + i + 1) % XS, y))

    def to_col(n, i, mine):
        src, dst, cut = parts[n]
        return remote(part(src if mine else dst, cut), part(dst, cut), col_send.at[n, i], tree_recv.at[n],
                      near(x, (y + i + 1) % YS))

    root = jnp.logical_and(x == rx, y == ry)
    mid = jnp.logical_and(x != rx, y == ry)

    @pl.when(root)
    def _():
        for n in range(3):
            for i in range(XS - 1):
                to_row(n, i).start()
            for i in range(YS - 1):
                to_col(n, i, True).start()
        a = pltpu.make_async_copy(freqs, tile_f.at[0], local_sem.at[0])
        b = pltpu.make_async_copy(small, tile_s.at[0], local_sem.at[1])
        a.start()
        b.start()
        a.wait()
        b.wait()

    def pass_on(n):
        @pl.when(mid)
        def _():
            to_row(n, 0).wait_recv()
            for i in range(YS - 1):
                to_col(n, i, False).start()

    def phi(i, src, sm, dst, base):
        block_ref = pack if i == 0 else points.at[i]

        def tile(j, _):
            cut = pl.ds(pl.multiple_of(j * 256, 256), 256)
            ang = jnp.dot(block_ref[0:block, :], src[:, cut], preferred_element_type=jnp.float32)
            to = pl.ds(pl.multiple_of(base + j * 256, 256), 256)
            dst[i * block:(i + 1) * block, to] = cos_turns(
                ang * TURN + sm[0:1, cut] * TURN, scale).astype(jnp.bfloat16)
            return 0

        lax.fori_loop(0, half // 256, tile, 0)

    def window(i):
        phi(i, freqs, small, wphi, own)
        phi(i, other_f, other_s, wphi, oth)
        block_ref = pack if i == 0 else points.at[i]
        tgt[:, i * block:(i + 1) * block] = block_ref[block:block + 8, :]

    def tiles(i):
        for j in range(2):
            phi(i, tile_f.at[j], tile_s.at[j], cphi, j * half)

    phi(0, freqs, small, wphi, own)
    tgt[:, 0:block] = pack[block:block + 8, :]
    ring_step(1)
    phi(1, freqs, small, wphi, own)
    pass_on(0)
    pass_on(1)
    pass_on(2)
    for copy in pair_copies:
        copy.wait_recv()
    phi(0, other_f, other_s, wphi, oth)
    phi(1, other_f, other_s, wphi, oth)
    tgt[:, block:2 * block] = points[1, block:block + 8, :]
    ring_step(2)
    for i in (2, 3):
        window(i)

    @pl.when(y != ry)
    def _():
        for n in range(3):
            to_col(n, 0, False).wait_recv()

    tile_copies = [
        go(remote(tile_s.at[0], tile_s.at[1], tile_send.at[0], tile_recv.at[0], mate)),
        go(remote(tile_f.at[0], tile_f.at[1], tile_send.at[1], tile_recv.at[1], mate)),
    ]
    window(4)
    ring_step(3)
    k0 = 4 * block
    for i in range(0, FB, 256):
        slab[i:i + 256, i:] = tdot(wphi[0:k0, i:i + 256], wphi[0:k0, i:])
    for i in (5, 6):
        window(i)
    for copy in tile_copies:
        copy.wait_recv()
    for i in range(0, 3):
        tiles(i)
    ring_step(4)
    window(7)

    def swap(n):
        cut = (pl.ds(n * 256, 256), pl.ds(n * 256, FB - n * 256))
        return remote(slab.at[cut], slab_in.at[cut], swap_send.at[n], swap_recv.at[n], mate)

    for n in range(4):
        i = n * 256
        slab[i:i + 256, i:] += tdot(wphi[k0:, i:i + 256], wphi[k0:, i:])
        if n > 0:
            swap(n - 1).start()
    tiles(3)
    swap(3).start()
    for i in range(4, 8):
        tiles(i)
    own_cut = pl.ds(own, half)
    gram_out[...] = tdot(wphi[:, own_cut], cphi[:, half:])
    proj[...] = jnp.dot(tgt[...], wphi[:, own_cut], preferred_element_type=jnp.float32)
    gram[...] = tdot(wphi[:, own_cut], cphi[:, 0:half])
    gram_copy = go(remote(gram_out, gram_in, swap_send.at[4], swap_recv.at[4], mate))
    proj_copy = remote(proj, proj_in, swap_send.at[5], swap_recv.at[5], mate)
    proj_copy.start()

    eye = lax.broadcasted_iota(jnp.int32, (NB, NB), 0) == lax.broadcasted_iota(jnp.int32, (NB, NB), 1)
    for n in range(4):
        swap(n).wait_send()
        swap(n).wait_recv()
        i = n * 256
        slab[i:i + 256, i:] += slab_in[i:i + 256, i:]
    for sm, base in ((small, own), (other_s, oth)):
        for i in range(0, half, NB):
            to = pl.ds(pl.multiple_of(base + i, NB), NB)
            slab[to, to] += jnp.where(eye, sm[1:2, i:i + NB], 0.0)
    gram_copy.wait_recv()
    gram[...] += gram_in[...]

    @pl.when(feat == data)
    def _():
        for i in range(0, half, NB):
            gram[i:i + NB, i:i + NB] += jnp.where(eye, small[1:2, i:i + NB], 0.0)

    proj_copy.wait_recv()
    proj_copy.wait_send()
    proj[...] += proj_in[...]

    @pl.when(root)
    def _():
        for n in range(3):
            for i in range(XS - 1):
                to_row(n, i).wait_send()

    @pl.when(y == ry)
    def _():
        for n in range(3):
            for i in range(YS - 1):
                to_col(n, i, False).wait_send()

    for copy in sends:
        copy.wait_send()


def assemble(scale, pack, freqs, small):
    dma = pltpu.SemaphoreType.DMA
    vmem = pl.BlockSpec(memory_space=pltpu.VMEM)
    f32, bf16 = jnp.float32, jnp.bfloat16
    half = freqs.shape[1]
    shape = jax.ShapeDtypeStruct
    rows = ZS * 256
    return pl.pallas_call(
        functools.partial(fused, scale),
        out_shape=(shape((FB, FB), f32), shape((half, half), f32), shape((8, half), f32)),
        in_specs=[vmem] * 3,
        out_specs=(vmem,) * 3,
        scratch_shapes=[
            pltpu.VMEM((ZS,) + pack.shape, bf16),
            pltpu.VMEM(freqs.shape, bf16), pltpu.VMEM(small.shape, f32),
            pltpu.VMEM((2,) + freqs.shape, bf16), pltpu.VMEM((2,) + small.shape, f32),
            pltpu.VMEM((rows, FB), bf16), pltpu.VMEM((rows, 2 * half), bf16), pltpu.VMEM((8, rows), bf16),
            pltpu.VMEM((FB, FB), f32), pltpu.VMEM((half, half), f32), pltpu.VMEM((half, half), f32),
            pltpu.VMEM((8, half), f32),
            dma((4, 2)), dma((4, 2)), dma((4, 2)), dma((4, 2)),
            dma((2,)), dma((2,)), dma((3,)), dma((3, 3)), dma((3, 3)),
            dma((2,)), dma((2,)), dma((6,)), dma((6,)), dma((2,)),
        ],
        compiler_params=pltpu.CompilerParams(
            collective_id=0, has_side_effects=True, vmem_limit_bytes=50 * 1024 * 1024),
    )(pack, freqs, small)


def chol(feat_axis, src, fac, slab, ue, ones, sem):
    half = fac.shape[0]
    odd = lax.rem(lax.axis_index(feat_axis), FB // half)
    own = pl.multiple_of(odd * half, half)
    loads = [
        pltpu.make_async_copy(src.at[pl.ds(i * NB, NB), pl.ds(i * NB, FB - i * NB)],
                              slab.at[pl.ds(i * NB, NB), pl.ds(i * NB, FB - i * NB)], sem.at[i])
        for i in range(FB // NB)
    ]
    for load in loads:
        load.start()
    for load in loads:
        load.wait()

    nblk = FB // NB
    ones[...] = jnp.ones_like(ones)

    def step(k, _):
        at = pl.multiple_of(k * NB, NB)
        blocks = [slab[pl.ds(pl.multiple_of(at + 8 * m, 8), 8), pl.ds(at, NB)] for m in range(NB // 8)]
        sub = lax.broadcasted_iota(jnp.int32, (8, NB), 0)
        lane = lax.broadcasted_iota(jnp.int32, (8, NB), 1)
        for m, (u, x) in enumerate(leaf(blocks, ones[...])):
            slab[pl.ds(pl.multiple_of(at + 8 * m, 8), 8), pl.ds(at, NB)] = jnp.where(lane >= sub + 8 * m, u, 0.0)
            ue[8 * m:8 * m + 8, :] = x
        for kk in range(nblk - 1):
            @pl.when(k == kk)
            def _():
                lo, mid = kk * NB, (kk + 1) * NB
                u12 = jnp.dot(ue[...], slab[lo:mid, mid:], precision=HI, preferred_element_type=jnp.float32)
                slab[lo:mid, mid:] = u12
                for i in range(mid, FB, 256):
                    w = min(256, FB - i)
                    slab[i:i + w, i:] -= tdot(u12[:, i - mid:i - mid + w], u12[:, i - mid:], HI)
        return 0

    lax.fori_loop(0, nblk, step, 0)

    for b in range(half // NB):
        for j in range(nblk):
            piece = jnp.transpose(slab[j * NB:(j + 1) * NB, pl.ds(pl.multiple_of(own + b * NB, NB), NB)])
            keep = j * NB <= own + b * NB
            fac[b * NB:(b + 1) * NB, j * NB:(j + 1) * NB] = jnp.where(keep, piece, 0.0)


def factor(slab):
    f32 = jnp.float32
    return pl.pallas_call(
        functools.partial(chol, "feat"),
        out_shape=jax.ShapeDtypeStruct((FB // 2, FB), f32),
        in_specs=[pl.BlockSpec(memory_space=pl.ANY)],
        out_specs=pl.BlockSpec(memory_space=pltpu.VMEM),
        scratch_shapes=[
            pltpu.VMEM((FB, FB), f32),
            pltpu.VMEM((NB, NB), f32),
            pltpu.VMEM((8, NB), f32),
            pltpu.SemaphoreType.DMA((FB // NB,)),
        ],
        compiler_params=pltpu.CompilerParams(vmem_limit_bytes=48 * 1024 * 1024),
    )(slab)


def shards(points, freqs, phase, ridge, targets):
    scale = math.sqrt(2.0 / (points.shape[0] * lax.axis_size("dp")))
    pack = jnp.pad(jnp.concatenate([points, targets], 0), ((0, 8), (0, 0)))
    slab, gram, proj = assemble(scale, pack, freqs, jnp.stack([phase, ridge]))
    return gram, proj, factor(slab)


def solution(mesh):
    in_specs = (P("dp", None), P(None, "feat"), P("feat"), P("feat"), P(None, "dp"))
    out_specs = (P("feat", "dp"), P(None, "feat"), P("feat", None))
    return jax.shard_map(shards, mesh=mesh, in_specs=in_specs, out_specs=out_specs, check_vma=False)
```

```python
import functools
import math

import jax
import jax.numpy as jnp
from jax import lax
from jax.experimental import pallas as pl
from jax.experimental.pallas import tpu as pltpu
from jax.sharding import PartitionSpec as P

FB = 1024
NB = 128
XS = 4
YS = 4
ZS = 8
HI = lax.Precision.HIGHEST
MESH = pl.DeviceIdType.MESH
TURN = 1.0 / (2.0 * math.pi)
C1, C3, C5, C7 = -6.283164044054801, 41.33714233314145, -81.34076747300007, 70.99341851060123


def cos_turns(turns, scale):
    r = turns - jnp.round(turns)
    u = jnp.abs(r) - 0.25
    w = u * u
    poly = ((C7 * scale * w + C5 * scale) * w + C3 * scale) * w + C1 * scale
    return poly * u


def tdot(left, right, precision=None):
    return lax.dot_general(
        left, right, (((0,), (0,)), ((), ())), precision=precision, preferred_element_type=jnp.float32
    )


def row_of(x, r):
    return jnp.broadcast_to(x[r:r + 1, :], x.shape)


def lane_of(x, c):
    return jnp.broadcast_to(x[:, c:c + 1], x.shape)


def leaf(blocks, one):
    n = NB // 8
    sub = lax.broadcasted_iota(jnp.int32, (8, NB), 0)
    lane = lax.broadcasted_iota(jnp.int32, (8, NB), 1)
    a = list(blocks)
    e = [jnp.where(lane == sub + 8 * m, 1.0, 0.0).astype(jnp.float32) for m in range(n)]

    def cols(m, k):
        return [lane_of(a[m], 8 * k + c) for c in range(8)]

    outs = []
    v, n1 = [x * one for x in cols(0, 0)], [x * one for x in cols(1, 0)]
    for k in range(n):
        pa, pe = a[k], e[k]
        has1, has2 = k + 1 < n, k + 2 < n
        far = {m: cols(m, k) for m in range(k + 2, n)}
        if has1:
            vn = cols(k + 1, k + 1)
        if has2:
            n2 = list(far[k + 2])
        rs = jnp.zeros((8, NB), jnp.float32)
        dv = jnp.zeros((8, NB), jnp.float32)
        for r in range(8):
            d = row_of(v[r], r)
            inv = 1.0 / d
            rs = jnp.where(sub == r, lax.rsqrt(d), rs)
            dv = jnp.where(sub == r, inv, dv)
            l = jnp.where(sub > r, v[r] * inv, 0.0)
            b = {c: row_of(v[c], r) for c in range(r + 1, 8)}
            ba, be = row_of(pa, r), row_of(pe, r)
            for c in b:
                v[c] = v[c] - l * b[c]
            pa = pa - l * ba
            pe = pe - l * be
            if has1:
                l1 = n1[r] * inv
                w = [row_of(n1[r], c) for c in range(8)]
                for c in b:
                    n1[c] = n1[c] - l1 * b[c]
                for c in range(8):
                    vn[c] = vn[c] - l1 * w[c]
                a[k + 1] = a[k + 1] - l1 * ba
                e[k + 1] = e[k + 1] - l1 * be
            if has2:
                l2 = n2[r] * inv
                for c in b:
                    n2[c] = n2[c] - l2 * b[c]
                a[k + 2] = a[k + 2] - l2 * ba
                e[k + 2] = e[k + 2] - l2 * be
        outs.append((pa * rs, pe * rs))
        if k + 3 < n:
            qa, qe = pa * dv, pe * dv
            for r in range(7, 0, -1):
                mult = jnp.where(sub < r, v[r] * dv, 0.0)
                qa = qa - mult * row_of(qa, r)
                qe = qe - mult * row_of(qe, r)
            ra = [row_of(qa, r) for r in range(8)]
            re = [row_of(qe, r) for r in range(8)]
            for m in range(k + 3, n):
                ma = [far[m][r] * ra[r] for r in range(8)]
                me = [far[m][r] * re[r] for r in range(8)]
                while len(ma) > 1:
                    ma = [ma[i] + ma[i + 1] for i in range(0, len(ma), 2)]
                    me = [me[i] + me[i + 1] for i in range(0, len(me), 2)]
                a[m] = a[m] - ma[0]
                e[m] = e[m] - me[0]
        if has1:
            v = vn
            if has2:
                n1 = [x * one for x in cols(k + 2, k + 1)]
    return outs


def fused(scale, pack, freqs, small, slab, gram, proj,
          points, other_f, other_s, tile_f, tile_s, wphi, cphi, tgt, slab_in, gram_out, gram_in, proj_in,
          up_send, up_recv, dn_send, dn_recv, pair_send, pair_recv, tree_recv, row_send, col_send,
          tile_send, tile_recv, swap_send, swap_recv, local_sem):
    data, feat = lax.axis_index("dp"), lax.axis_index("feat")
    z, core = data // 2, data % 2
    x, y = feat // YS, feat % YS
    block, half = 256, freqs.shape[1]
    odd = feat % 2
    own = pl.multiple_of(odd * half, half)
    oth = pl.multiple_of((1 - odd) * half, half)

    def at(zz, cc):
        return {"dp": zz * 2 + cc, "feat": feat}

    def near(xx, yy):
        return {"dp": data, "feat": xx * YS + yy}

    up, dn, mate = at((z + 1) % ZS, core), at((z + ZS - 1) % ZS, core), at(z, 1 - core)
    barrier = pltpu.get_barrier_semaphore()
    peers = [up, dn, mate]
    peers += [near((x + i) % XS, y) for i in range(1, XS)] + [near(x, (y + i) % YS) for i in range(1, YS)]
    for peer in peers:
        pl.semaphore_signal(barrier, inc=1, device_id=peer, device_id_type=MESH)
    pl.semaphore_wait(barrier, len(peers))

    first = 128
    pieces = (pl.ds(0, first), pl.ds(first, pack.shape[0] - first))
    sends = []

    def remote(src, dst, ssem, rsem, where):
        return pltpu.make_async_remote_copy(
            src_ref=src, dst_ref=dst, send_sem=ssem, recv_sem=rsem, device_id=where, device_id_type=MESH)

    def go(copy):
        copy.start()
        sends.append(copy)
        return copy

    def arrival(step, upward):
        return 7 if step == 4 else 2 * step - (1 if upward else 0)

    def ring(step, p, upward):
        src = pack if step == 0 else points.at[arrival(step, upward)]
        dst = points.at[arrival(step + 1, upward)]
        ssem, rsem, where = (up_send, up_recv, up) if upward else (dn_send, dn_recv, dn)
        return remote(src.at[pieces[p]], dst.at[pieces[p]], ssem.at[step, p], rsem.at[step, p], where)

    def ring_step(step):
        todo = [(0, True), (0, False), (1, True), (1, False)] if step < 4 else [(0, True), (1, False)]
        for p, upward in todo:
            ring(step - 1, p, upward).wait_recv()
            if step < 3 or (step == 3 and p == (0 if upward else 1)):
                go(ring(step, p, upward))

    for p in range(2):
        go(ring(0, p, True))
        go(ring(0, p, False))
    pair = near(x, y + 1 - 2 * (y % 2))
    pair_copies = [
        go(remote(small, other_s, pair_send.at[0], pair_recv.at[0], pair)),
        go(remote(freqs, other_f, pair_send.at[1], pair_recv.at[1], pair)),
    ]

    rx, ry = data // YS, data % YS
    parts = [(small, tile_s.at[0], None), (freqs, tile_f.at[0], pl.ds(0, 128)), (freqs, tile_f.at[0], pl.ds(128, 128))]

    def part(ref, cut):
        return ref if cut is None else ref.at[cut]

    def to_row(n, i):
        src, dst, cut = parts[n]
        return remote(part(src, cut), part(dst, cut), row_send.at[n, i], tree_recv.at[n], near((x + i + 1) % XS, y))

    def to_col(n, i, mine):
        src, dst, cut = parts[n]
        return remote(part(src if mine else dst, cut), part(dst, cut), col_send.at[n, i], tree_recv.at[n],
                      near(x, (y + i + 1) % YS))

    root = jnp.logical_and(x == rx, y == ry)
    mid = jnp.logical_and(x != rx, y == ry)

    @pl.when(root)
    def _():
        for n in range(3):
            for i in range(XS - 1):
                to_row(n, i).start()
            for i in range(YS - 1):
                to_col(n, i, True).start()
        a = pltpu.make_async_copy(freqs, tile_f.at[0], local_sem.at[0])
        b = pltpu.make_async_copy(small, tile_s.at[0], local_sem.at[1])
        a.start()
        b.start()
        a.wait()
        b.wait()

    def pass_on(n):
        @pl.when(mid)
        def _():
            to_row(n, 0).wait_recv()
            for i in range(YS - 1):
                to_col(n, i, False).start()

    def phi(i, src, sm, dst, base):
        block_ref = pack if i == 0 else points.at[i]

        def tile(j, _):
            cut = pl.ds(pl.multiple_of(j * 256, 256), 256)
            ang = jnp.dot(block_ref[0:block, :], src[:, cut], preferred_element_type=jnp.float32)
            to = pl.ds(pl.multiple_of(base + j * 256, 256), 256)
            dst[i * block:(i + 1) * block, to] = cos_turns(
                ang * TURN + sm[0:1, cut] * TURN, scale).astype(jnp.bfloat16)
            return 0

        lax.fori_loop(0, half // 256, tile, 0)

    def window(i):
        phi(i, freqs, small, wphi, own)
        phi(i, other_f, other_s, wphi, oth)
        block_ref = pack if i == 0 else points.at[i]
        tgt[:, i * block:(i + 1) * block] = block_ref[block:block + 8, :]

    def tiles(i):
        for j in range(2):
            phi(i, tile_f.at[j], tile_s.at[j], cphi, j * half)

    phi(0, freqs, small, wphi, own)
    tgt[:, 0:block] = pack[block:block + 8, :]
    ring_step(1)
    phi(1, freqs, small, wphi, own)
    pass_on(0)
    pass_on(1)
    pass_on(2)
    for copy in pair_copies:
        copy.wait_recv()
    phi(0, other_f, other_s, wphi, oth)
    phi(1, other_f, other_s, wphi, oth)
    tgt[:, block:2 * block] = points[1, block:block + 8, :]
    ring_step(2)
    for i in (2, 3):
        window(i)

    @pl.when(y != ry)
    def _():
        for n in range(3):
            to_col(n, 0, False).wait_recv()

    tile_copies = [
        go(remote(tile_s.at[0], tile_s.at[1], tile_send.at[0], tile_recv.at[0], mate)),
        go(remote(tile_f.at[0], tile_f.at[1], tile_send.at[1], tile_recv.at[1], mate)),
    ]
    window(4)
    ring_step(3)
    k0 = 4 * block
    for i in range(0, FB, 256):
        slab[i:i + 256, i:] = tdot(wphi[0:k0, i:i + 256], wphi[0:k0, i:])
    for i in (5, 6):
        window(i)
    for copy in tile_copies:
        copy.wait_recv()
    for i in range(0, 3):
        tiles(i)
    ring_step(4)
    window(7)

    def swap(n):
        cut = (pl.ds(n * 256, 256), pl.ds(n * 256, FB - n * 256))
        return remote(slab.at[cut], slab_in.at[cut], swap_send.at[n], swap_recv.at[n], mate)

    for n in range(4):
        i = n * 256
        slab[i:i + 256, i:] += tdot(wphi[k0:, i:i + 256], wphi[k0:, i:])
        if n > 0:
            swap(n - 1).start()
    tiles(3)
    swap(3).start()
    for i in range(4, 8):
        tiles(i)
    own_cut = pl.ds(own, half)
    gram_out[...] = tdot(wphi[:, own_cut], cphi[:, half:])
    proj[...] = jnp.dot(tgt[...], wphi[:, own_cut], preferred_element_type=jnp.float32)
    gram[...] = tdot(wphi[:, own_cut], cphi[:, 0:half])
    gram_copy = go(remote(gram_out, gram_in, swap_send.at[4], swap_recv.at[4], mate))
    proj_copy = remote(proj, proj_in, swap_send.at[5], swap_recv.at[5], mate)
    proj_copy.start()

    eye = lax.broadcasted_iota(jnp.int32, (NB, NB), 0) == lax.broadcasted_iota(jnp.int32, (NB, NB), 1)
    for n in range(4):
        swap(n).wait_send()
        swap(n).wait_recv()
        i = n * 256
        slab[i:i + 256, i:] += slab_in[i:i + 256, i:]
    for sm, base in ((small, own), (other_s, oth)):
        for i in range(0, half, NB):
            to = pl.ds(pl.multiple_of(base + i, NB), NB)
            slab[to, to] += jnp.where(eye, sm[1:2, i:i + NB], 0.0)
    gram_copy.wait_recv()
    gram[...] += gram_in[...]

    @pl.when(feat == data)
    def _():
        for i in range(0, half, NB):
            gram[i:i + NB, i:i + NB] += jnp.where(eye, small[1:2, i:i + NB], 0.0)

    proj_copy.wait_recv()
    proj_copy.wait_send()
    proj[...] += proj_in[...]

    @pl.when(root)
    def _():
        for n in range(3):
            for i in range(XS - 1):
                to_row(n, i).wait_send()

    @pl.when(y == ry)
    def _():
        for n in range(3):
            for i in range(YS - 1):
                to_col(n, i, False).wait_send()

    for copy in sends:
        copy.wait_send()


def assemble(scale, pack, freqs, small):
    dma = pltpu.SemaphoreType.DMA
    vmem = pl.BlockSpec(memory_space=pltpu.VMEM)
    f32, bf16 = jnp.float32, jnp.bfloat16
    half = freqs.shape[1]
    shape = jax.ShapeDtypeStruct
    rows = ZS * 256
    return pl.pallas_call(
        functools.partial(fused, scale),
        out_shape=(shape((FB, FB), f32), shape((half, half), f32), shape((8, half), f32)),
        in_specs=[vmem] * 3,
        out_specs=(vmem,) * 3,
        scratch_shapes=[
            pltpu.VMEM((ZS,) + pack.shape, bf16),
            pltpu.VMEM(freqs.shape, bf16), pltpu.VMEM(small.shape, f32),
            pltpu.VMEM((2,) + freqs.shape, bf16), pltpu.VMEM((2,) + small.shape, f32),
            pltpu.VMEM((rows, FB), bf16), pltpu.VMEM((rows, 2 * half), bf16), pltpu.VMEM((8, rows), bf16),
            pltpu.VMEM((FB, FB), f32), pltpu.VMEM((half, half), f32), pltpu.VMEM((half, half), f32),
            pltpu.VMEM((8, half), f32),
            dma((4, 2)), dma((4, 2)), dma((4, 2)), dma((4, 2)),
            dma((2,)), dma((2,)), dma((3,)), dma((3, 3)), dma((3, 3)),
            dma((2,)), dma((2,)), dma((6,)), dma((6,)), dma((2,)),
        ],
        compiler_params=pltpu.CompilerParams(
            collective_id=0, has_side_effects=True, vmem_limit_bytes=32 * 1024 * 1024),
    )(pack, freqs, small)


def three(x):
    hi = x.astype(jnp.bfloat16)
    rest = x - hi.astype(jnp.float32)
    mid = rest.astype(jnp.bfloat16)
    return hi, mid, (rest - mid.astype(jnp.float32)).astype(jnp.bfloat16)


def left_terms(x):
    h, m, l = three(x)
    return jnp.concatenate([h, h, m, h, l, m], axis=1)


def right_terms(x):
    h, m, l = three(x)
    return jnp.concatenate([h, m, h, l, h, m], axis=0)


def chol(feat_axis, src, gram_src, proj_src, fac, slab, gram, proj, facv, ue, ones, sem):
    half = facv.shape[0]
    odd = lax.rem(lax.axis_index(feat_axis), FB // half)
    own = pl.multiple_of(odd * half, half)
    nblk = FB // NB
    through = [pltpu.make_async_copy(gram_src, gram, sem.at[nblk]), pltpu.make_async_copy(proj_src, proj, sem.at[nblk + 1])]
    for copy in through:
        copy.start()
    ones[...] = jnp.ones_like(ones)

    def column(k):
        cut = pl.ds(pl.multiple_of(k * NB, NB), NB)
        return pltpu.make_async_copy(facv.at[:, cut], fac.at[:, cut], sem.at[k])

    def step(k, _):
        at = pl.multiple_of(k * NB, NB)
        blocks = [slab[pl.ds(pl.multiple_of(at + 8 * m, 8), 8), pl.ds(at, NB)] for m in range(NB // 8)]
        sub = lax.broadcasted_iota(jnp.int32, (8, NB), 0)
        lane = lax.broadcasted_iota(jnp.int32, (8, NB), 1)
        for m, (u, x) in enumerate(leaf(blocks, ones[...])):
            slab[pl.ds(pl.multiple_of(at + 8 * m, 8), 8), pl.ds(at, NB)] = jnp.where(lane >= sub + 8 * m, u, 0.0)
            ue[8 * m:8 * m + 8, :] = x
        for kk in range(nblk - 1):
            @pl.when(k == kk)
            def _():
                lo, mid = kk * NB, (kk + 1) * NB
                u12 = jnp.dot(left_terms(ue[...]), right_terms(slab[lo:mid, mid:]), preferred_element_type=jnp.float32)
                slab[lo:mid, mid:] = u12
                left, right = left_terms(jnp.transpose(u12)), right_terms(u12)
                for i in range(0, FB - mid, 256):
                    w = min(256, FB - mid - i)
                    slab[mid + i:mid + i + w, mid + i:] -= jnp.dot(
                        left[i:i + w], right[:, i:], preferred_element_type=jnp.float32)
        for b in range(half // NB):
            piece = jnp.transpose(slab[pl.ds(at, NB), pl.ds(pl.multiple_of(own + b * NB, NB), NB)])
            facv[b * NB:(b + 1) * NB, pl.ds(at, NB)] = jnp.where(at <= own + b * NB, piece, 0.0)
        column(k).start()
        return 0

    lax.fori_loop(0, nblk, step, 0)
    for k in range(nblk):
        column(k).wait()
    for copy in through:
        copy.wait()


def factor(slab, gram, proj, flags=None):
    f32 = jnp.float32
    hold = pl.BlockSpec(memory_space=pl.ANY)
    vmem = pl.BlockSpec(memory_space=pltpu.VMEM)
    shape = jax.ShapeDtypeStruct
    fac, _, gram, proj = pl.pallas_call(
        functools.partial(chol, "feat"),
        out_shape=(shape((FB // 2, FB), f32), shape(slab.shape, f32), shape(gram.shape, f32), shape(proj.shape, f32)),
        in_specs=[vmem, hold, hold],
        out_specs=(hold, vmem, hold, hold),
        input_output_aliases={0: 1},
        scratch_shapes=[
            pltpu.VMEM((FB // 2, FB), f32),
            pltpu.VMEM((NB, NB), f32),
            pltpu.VMEM((8, NB), f32),
            pltpu.SemaphoreType.DMA((FB // NB + 2,)),
        ],
        compiler_params=pltpu.CompilerParams(vmem_limit_bytes=20 * 1024 * 1024, flags=flags),
    )(slab, gram, proj)
    return gram, proj, fac


def shards(points, freqs, phase, ridge, targets):
    scale = math.sqrt(2.0 / (points.shape[0] * lax.axis_size("dp")))
    pack = jnp.pad(jnp.concatenate([points, targets], 0), ((0, 8), (0, 0)))
    slab, gram, proj = assemble(scale, pack, freqs, jnp.stack([phase, ridge]))
    return factor(slab, gram, proj)


def solution(mesh):
    in_specs = (P("dp", None), P(None, "feat"), P("feat"), P("feat"), P(None, "dp"))
    out_specs = (P("feat", "dp"), P(None, "feat"), P("feat", None))
    return jax.shard_map(shards, mesh=mesh, in_specs=in_specs, out_specs=out_specs, check_vma=False)
```

```python
import functools
import math

import jax
import jax.numpy as jnp
from jax import lax
from jax.experimental import pallas as pl
from jax.experimental.pallas import tpu as pltpu
from jax.sharding import PartitionSpec as P

FB = 1024
NB = 128
XS = 4
YS = 4
ZS = 8
PIECES = 4
HI = lax.Precision.HIGHEST
MESH = pl.DeviceIdType.MESH
TURN = 1.0 / (2.0 * math.pi)
C1, C3, C5, C7 = -6.283164044054801, 41.33714233314145, -81.34076747300007, 70.99341851060123


def cos_turns(turns, scale):
    r = turns - jnp.round(turns)
    u = jnp.abs(r) - 0.25
    w = u * u
    poly = ((C7 * scale * w + C5 * scale) * w + C3 * scale) * w + C1 * scale
    return poly * u


def tdot(left, right, precision=None):
    return lax.dot_general(
        left, right, (((0,), (0,)), ((), ())), precision=precision, preferred_element_type=jnp.float32
    )


def row_of(x, r):
    return jnp.broadcast_to(x[r:r + 1, :], x.shape)


def lane_of(x, c):
    return jnp.broadcast_to(x[:, c:c + 1], x.shape)


def leaf(blocks, one):
    n = NB // 8
    sub = lax.broadcasted_iota(jnp.int32, (8, NB), 0)
    lane = lax.broadcasted_iota(jnp.int32, (8, NB), 1)
    a = list(blocks)
    e = [jnp.where(lane == sub + 8 * m, 1.0, 0.0).astype(jnp.float32) for m in range(n)]

    def cols(m, k):
        return [lane_of(a[m], 8 * k + c) for c in range(8)]

    outs = []
    v, n1 = [x * one for x in cols(0, 0)], [x * one for x in cols(1, 0)]
    for k in range(n):
        pa, pe = a[k], e[k]
        has1, has2 = k + 1 < n, k + 2 < n
        far = {m: cols(m, k) for m in range(k + 2, n)}
        if has1:
            vn = cols(k + 1, k + 1)
        if has2:
            n2 = list(far[k + 2])
        rs = jnp.zeros((8, NB), jnp.float32)
        dv = jnp.zeros((8, NB), jnp.float32)
        for r in range(8):
            d = row_of(v[r], r)
            inv = 1.0 / d
            rs = jnp.where(sub == r, lax.rsqrt(d), rs)
            dv = jnp.where(sub == r, inv, dv)
            l = jnp.where(sub > r, v[r] * inv, 0.0)
            b = {c: row_of(v[c], r) for c in range(r + 1, 8)}
            ba, be = row_of(pa, r), row_of(pe, r)
            for c in b:
                v[c] = v[c] - l * b[c]
            pa = pa - l * ba
            pe = pe - l * be
            if has1:
                l1 = n1[r] * inv
                w = [row_of(n1[r], c) for c in range(8)]
                for c in b:
                    n1[c] = n1[c] - l1 * b[c]
                for c in range(8):
                    vn[c] = vn[c] - l1 * w[c]
                a[k + 1] = a[k + 1] - l1 * ba
                e[k + 1] = e[k + 1] - l1 * be
            if has2:
                l2 = n2[r] * inv
                for c in b:
                    n2[c] = n2[c] - l2 * b[c]
                a[k + 2] = a[k + 2] - l2 * ba
                e[k + 2] = e[k + 2] - l2 * be
        outs.append((pa * rs, pe * rs))
        if k + 3 < n:
            qa, qe = pa * dv, pe * dv
            for r in range(7, 0, -1):
                mult = jnp.where(sub < r, v[r] * dv, 0.0)
                qa = qa - mult * row_of(qa, r)
                qe = qe - mult * row_of(qe, r)
            ra = [row_of(qa, r) for r in range(8)]
            re = [row_of(qe, r) for r in range(8)]
            for m in range(k + 3, n):
                ma = [far[m][r] * ra[r] for r in range(8)]
                me = [far[m][r] * re[r] for r in range(8)]
                while len(ma) > 1:
                    ma = [ma[i] + ma[i + 1] for i in range(0, len(ma), 2)]
                    me = [me[i] + me[i + 1] for i in range(0, len(me), 2)]
                a[m] = a[m] - ma[0]
                e[m] = e[m] - me[0]
        if has1:
            v = vn
            if has2:
                n1 = [x * one for x in cols(k + 2, k + 1)]
    return outs


def fused(scale, pack, freqs, small, slab, gram, proj,
          points, other_f, other_s, tile_f, tile_s, wphi, cphi, tgt, slab_in, gram_out, gram_in, proj_part, proj_in,
          up_send, up_recv, dn_send, dn_recv, pair_send, pair_recv, tree_recv, row_send, col_send,
          tile_send, tile_recv, swap_send, swap_recv, local_sem):
    data, feat = lax.axis_index("dp"), lax.axis_index("feat")
    z, core = data // 2, data % 2
    x, y = feat // YS, feat % YS
    block, half = 256, freqs.shape[1]
    odd = feat % 2
    own = pl.multiple_of(odd * half, half)
    oth = pl.multiple_of((1 - odd) * half, half)

    def at(zz, cc):
        return {"dp": zz * 2 + cc, "feat": feat}

    def near(xx, yy):
        return {"dp": data, "feat": xx * YS + yy}

    up, dn, mate = at((z + 1) % ZS, core), at((z + ZS - 1) % ZS, core), at(z, 1 - core)
    barrier = pltpu.get_barrier_semaphore()
    peers = [up, dn, mate]
    peers += [near((x + i) % XS, y) for i in range(1, XS)] + [near(x, (y + i) % YS) for i in range(1, YS)]
    for peer in peers:
        pl.semaphore_signal(barrier, inc=1, device_id=peer, device_id_type=MESH)
    pl.semaphore_wait(barrier, len(peers))

    count = up_send.shape[1]
    cuts = [i * (block // count) for i in range(count)] + [pack.shape[0]]
    pieces = [pl.ds(lo, hi - lo) for lo, hi in zip(cuts[:-1], cuts[1:])]
    sends = []

    def remote(src, dst, ssem, rsem, where):
        return pltpu.make_async_remote_copy(
            src_ref=src, dst_ref=dst, send_sem=ssem, recv_sem=rsem, device_id=where, device_id_type=MESH)

    def go(copy):
        copy.start()
        sends.append(copy)
        return copy

    def arrival(step, upward):
        return 7 if step == 4 else 2 * step - (1 if upward else 0)

    def ring(step, p, upward):
        src = pack if step == 0 else points.at[arrival(step, upward)]
        dst = points.at[arrival(step + 1, upward)]
        ssem, rsem, where = (up_send, up_recv, up) if upward else (dn_send, dn_recv, dn)
        return remote(src.at[pieces[p]], dst.at[pieces[p]], ssem.at[step, p], rsem.at[step, p], where)

    def ring_step(step):
        for p in range(count):
            for upward in (True, False):
                mine = (p < count // 2) == upward
                if step == 4 and not mine:
                    continue
                ring(step - 1, p, upward).wait_recv()
                if step < 3 or (step == 3 and mine):
                    go(ring(step, p, upward))

    for p in range(count):
        go(ring(0, p, True))
        go(ring(0, p, False))
    pair = near(x, y + 1 - 2 * (y % 2))
    part_rows = freqs.shape[0] // 2
    here = pl.ds(pl.multiple_of(core * part_rows, part_rows), part_rows)
    pair_copies = [
        go(remote(small, other_s, pair_send.at[0], pair_recv.at[0], pair)),
        go(remote(freqs.at[here], other_f.at[here], pair_send.at[1], pair_recv.at[1], pair)),
    ]

    def pair_ready():
        for copy in pair_copies:
            copy.wait_recv()
        return go(remote(other_f.at[here], other_f.at[here], pair_send.at[2], pair_recv.at[2], mate))

    rx, ry = data // YS, data % YS
    parts = [(small, tile_s.at[0], None), (freqs, tile_f.at[0], pl.ds(0, 128)), (freqs, tile_f.at[0], pl.ds(128, 128))]

    def part(ref, cut):
        return ref if cut is None else ref.at[cut]

    def to_row(n, i):
        src, dst, cut = parts[n]
        return remote(part(src, cut), part(dst, cut), row_send.at[n, i], tree_recv.at[n], near((x + i + 1) % XS, y))

    def to_col(n, i, mine):
        src, dst, cut = parts[n]
        return remote(part(src if mine else dst, cut), part(dst, cut), col_send.at[n, i], tree_recv.at[n],
                      near(x, (y + i + 1) % YS))

    root = jnp.logical_and(x == rx, y == ry)
    mid = jnp.logical_and(x != rx, y == ry)

    @pl.when(root)
    def _():
        for n in range(3):
            for i in range(XS - 1):
                to_row(n, i).start()
            for i in range(YS - 1):
                to_col(n, i, True).start()
        a = pltpu.make_async_copy(freqs, tile_f.at[0], local_sem.at[0])
        b = pltpu.make_async_copy(small, tile_s.at[0], local_sem.at[1])
        a.start()
        b.start()
        a.wait()
        b.wait()

    def pass_on(n):
        @pl.when(mid)
        def _():
            to_row(n, 0).wait_recv()
            for i in range(YS - 1):
                to_col(n, i, False).start()

    def phi(i, src, sm, dst, base):
        block_ref = pack if i == 0 else points.at[i]

        for j in range(0, half, 256):
            ang = jnp.dot(block_ref[0:block, :], src[:, j:j + 256], preferred_element_type=jnp.float32)
            to = pl.ds(pl.multiple_of(base + j, 256), 256)
            dst[i * block:(i + 1) * block, to] = cos_turns(
                ang * TURN + sm[0:1, j:j + 256] * TURN, scale).astype(jnp.bfloat16)

    def mine(i):
        phi(i, freqs, small, wphi, own)
        block_ref = pack if i == 0 else points.at[i]
        tgt[:, i * block:(i + 1) * block] = block_ref[block:block + 8, :]

    def others(i):
        phi(i, other_f, other_s, wphi, oth)

    def tiles(i):
        for j in range(2):
            phi(i, tile_f.at[j], tile_s.at[j], cphi, j * half)

    def swap(n):
        cut = (pl.ds(n * 256, 256), pl.ds(n * 256, FB - n * 256))
        return remote(slab.at[cut], slab_in.at[cut], swap_send.at[n], swap_recv.at[n], mate)

    mine(0)
    ring_step(1)
    mine(1)
    mine(2)
    pass_on(0)
    pass_on(1)
    ring_step(2)
    pass_on(2)
    from_mate = pair_ready()
    mine(3)
    mine(4)
    from_mate.wait_recv()
    for i in range(3):
        others(i)
    ring_step(3)
    for i in (3, 4):
        others(i)
    for i in (5, 6):
        mine(i)
        others(i)

    @pl.when(y != ry)
    def _():
        for n in range(3):
            to_col(n, 0, False).wait_recv()

    tile_copies = [
        go(remote(tile_s.at[0], tile_s.at[1], tile_send.at[0], tile_recv.at[0], mate)),
        go(remote(tile_f.at[0], tile_f.at[1], tile_send.at[1], tile_recv.at[1], mate)),
    ]
    k0 = 6 * block
    for i in range(0, FB, 256):
        slab[i:i + 256, i:] = tdot(wphi[0:k0, i:i + 256], wphi[0:k0, i:])
    for copy in tile_copies:
        copy.wait_recv()
    for i in range(4):
        tiles(i)
    ring_step(4)
    mine(7)
    others(7)
    for n in range(4):
        i = n * 256
        slab[i:i + 256, i:] += tdot(wphi[k0:, i:i + 256], wphi[k0:, i:])
        if n > 0:
            swap(n - 1).start()
    own_cut = pl.ds(own, half)
    proj_part[...] = jnp.dot(tgt[...], wphi[:, own_cut], preferred_element_type=jnp.float32)
    swap(3).start()
    for i in range(4, 8):
        phi(i, tile_f.at[1], tile_s.at[1], cphi, half)
    proj_copy = go(remote(proj_part, proj_in, swap_send.at[5], swap_recv.at[5], mate))
    gram_out[...] = tdot(wphi[:, own_cut], cphi[:, half:])
    for i in range(4, 8):
        phi(i, tile_f.at[0], tile_s.at[0], cphi, 0)
    gram_copy = go(remote(gram_out, gram_in, swap_send.at[4], swap_recv.at[4], mate))
    gram[...] = tdot(wphi[:, own_cut], cphi[:, 0:half])

    eye = lax.broadcasted_iota(jnp.int32, (NB, NB), 0) == lax.broadcasted_iota(jnp.int32, (NB, NB), 1)
    for n in range(4):
        swap(n).wait_send()
        swap(n).wait_recv()
        i = n * 256
        slab[i:i + 256, i:] += slab_in[i:i + 256, i:]
    for sm, base in ((small, own), (other_s, oth)):
        for i in range(0, half, NB):
            to = pl.ds(pl.multiple_of(base + i, NB), NB)
            slab[to, to] += jnp.where(eye, sm[1:2, i:i + NB], 0.0)
    gram_copy.wait_recv()
    gram[...] += gram_in[...]

    @pl.when(feat == data)
    def _():
        for i in range(0, half, NB):
            gram[i:i + NB, i:i + NB] += jnp.where(eye, small[1:2, i:i + NB], 0.0)

    proj_copy.wait_recv()
    proj[...] = proj_part[...] + proj_in[...]

    @pl.when(root)
    def _():
        for n in range(3):
            for i in range(XS - 1):
                to_row(n, i).wait_send()

    @pl.when(y == ry)
    def _():
        for n in range(3):
            for i in range(YS - 1):
                to_col(n, i, False).wait_send()

    for copy in sends:
        copy.wait_send()


def assemble(scale, pack, freqs, small):
    dma = pltpu.SemaphoreType.DMA
    vmem = pl.BlockSpec(memory_space=pltpu.VMEM)
    f32, bf16 = jnp.float32, jnp.bfloat16
    half = freqs.shape[1]
    shape = jax.ShapeDtypeStruct
    rows = ZS * 256
    return pl.pallas_call(
        functools.partial(fused, scale),
        out_shape=(shape((FB, FB), f32), shape((half, half), f32), shape((8, half), f32)),
        in_specs=[vmem] * 3,
        out_specs=(vmem,) * 3,
        scratch_shapes=[
            pltpu.VMEM((ZS,) + pack.shape, bf16),
            pltpu.VMEM(freqs.shape, bf16), pltpu.VMEM(small.shape, f32),
            pltpu.VMEM((2,) + freqs.shape, bf16), pltpu.VMEM((2,) + small.shape, f32),
            pltpu.VMEM((rows, FB), bf16), pltpu.VMEM((rows, 2 * half), bf16), pltpu.VMEM((8, rows), bf16),
            pltpu.VMEM((FB, FB), f32), pltpu.VMEM((half, half), f32), pltpu.VMEM((half, half), f32),
            pltpu.VMEM((8, half), f32), pltpu.VMEM((8, half), f32),
            dma((4, PIECES)), dma((4, PIECES)), dma((4, PIECES)), dma((4, PIECES)),
            dma((3,)), dma((3,)), dma((3,)), dma((3, 3)), dma((3, 3)),
            dma((2,)), dma((2,)), dma((6,)), dma((6,)), dma((2,)),
        ],
        compiler_params=pltpu.CompilerParams(
            collective_id=0, has_side_effects=True, vmem_limit_bytes=32 * 1024 * 1024),
    )(pack, freqs, small)


def three(x):
    hi = x.astype(jnp.bfloat16)
    rest = x - hi.astype(jnp.float32)
    mid = rest.astype(jnp.bfloat16)
    return hi, mid, (rest - mid.astype(jnp.float32)).astype(jnp.bfloat16)


def left_terms(x):
    h, m, l = three(x)
    return jnp.concatenate([h, h, m, h, l, m], axis=1)


def right_terms(x):
    h, m, l = three(x)
    return jnp.concatenate([h, m, h, l, h, m], axis=0)


def chol(feat_axis, src, gram_src, proj_src, fac, slab, gram, proj, facv, ue, ones, sem):
    half = facv.shape[0]
    odd = lax.rem(lax.axis_index(feat_axis), FB // half)
    own = pl.multiple_of(odd * half, half)
    nblk = FB // NB
    through = [pltpu.make_async_copy(gram_src, gram, sem.at[nblk]), pltpu.make_async_copy(proj_src, proj, sem.at[nblk + 1])]
    for copy in through:
        copy.start()
    ones[...] = jnp.ones_like(ones)

    def column(k):
        cut = pl.ds(pl.multiple_of(k * NB, NB), NB)
        return pltpu.make_async_copy(facv.at[:, cut], fac.at[:, cut], sem.at[k])

    def step(k, _):
        at = pl.multiple_of(k * NB, NB)
        blocks = [slab[pl.ds(pl.multiple_of(at + 8 * m, 8), 8), pl.ds(at, NB)] for m in range(NB // 8)]
        sub = lax.broadcasted_iota(jnp.int32, (8, NB), 0)
        lane = lax.broadcasted_iota(jnp.int32, (8, NB), 1)
        for m, (u, x) in enumerate(leaf(blocks, ones[...])):
            slab[pl.ds(pl.multiple_of(at + 8 * m, 8), 8), pl.ds(at, NB)] = jnp.where(lane >= sub + 8 * m, u, 0.0)
            ue[8 * m:8 * m + 8, :] = x
        for kk in range(nblk - 1):
            @pl.when(k == kk)
            def _():
                lo, mid = kk * NB, (kk + 1) * NB
                u12 = jnp.dot(left_terms(ue[...]), right_terms(slab[lo:mid, mid:]), preferred_element_type=jnp.float32)
                slab[lo:mid, mid:] = u12
                left, right = left_terms(jnp.transpose(u12)), right_terms(u12)
                for i in range(0, FB - mid, 256):
                    w = min(256, FB - mid - i)
                    slab[mid + i:mid + i + w, mid + i:] -= jnp.dot(
                        left[i:i + w], right[:, i:], preferred_element_type=jnp.float32)
        for b in range(half // NB):
            piece = jnp.transpose(slab[pl.ds(at, NB), pl.ds(pl.multiple_of(own + b * NB, NB), NB)])
            facv[b * NB:(b + 1) * NB, pl.ds(at, NB)] = jnp.where(at <= own + b * NB, piece, 0.0)
        column(k).start()
        return 0

    lax.fori_loop(0, nblk, step, 0)
    for k in range(nblk):
        column(k).wait()
    for copy in through:
        copy.wait()


def factor(slab, gram, proj, flags=None):
    f32 = jnp.float32
    hold = pl.BlockSpec(memory_space=pl.ANY)
    vmem = pl.BlockSpec(memory_space=pltpu.VMEM)
    shape = jax.ShapeDtypeStruct
    fac, _, gram, proj = pl.pallas_call(
        functools.partial(chol, "feat"),
        out_shape=(shape((FB // 2, FB), f32), shape(slab.shape, f32), shape(gram.shape, f32), shape(proj.shape, f32)),
        in_specs=[vmem, hold, hold],
        out_specs=(hold, vmem, hold, hold),
        input_output_aliases={0: 1},
        scratch_shapes=[
            pltpu.VMEM((FB // 2, FB), f32),
            pltpu.VMEM((NB, NB), f32),
            pltpu.VMEM((8, NB), f32),
            pltpu.SemaphoreType.DMA((FB // NB + 2,)),
        ],
        compiler_params=pltpu.CompilerParams(vmem_limit_bytes=20 * 1024 * 1024, flags=flags),
    )(slab, gram, proj)
    return gram, proj, fac


def shards(points, freqs, phase, ridge, targets):
    scale = math.sqrt(2.0 / (points.shape[0] * lax.axis_size("dp")))
    pack = jnp.pad(jnp.concatenate([points, targets], 0), ((0, 8), (0, 0)))
    slab, gram, proj = assemble(scale, pack, freqs, jnp.stack([phase, ridge]))
    return factor(slab, gram, proj)


def solution(mesh):
    in_specs = (P("dp", None), P(None, "feat"), P("feat"), P("feat"), P(None, "dp"))
    out_specs = (P("feat", "dp"), P(None, "feat"), P("feat", None))
    return jax.shard_map(shards, mesh=mesh, in_specs=in_specs, out_specs=out_specs, check_vma=False)
```

```python
import functools
import math

import jax
import jax.numpy as jnp
from jax import lax
from jax.experimental import pallas as pl
from jax.experimental.pallas import tpu as pltpu
from jax.sharding import PartitionSpec as P

FB = 1024
NB = 128
XS = 4
YS = 4
ZS = 8
PIECES = 4
HI = lax.Precision.HIGHEST
MESH = pl.DeviceIdType.MESH
TURN = 1.0 / (2.0 * math.pi)
C1, C3, C5, C7 = -6.283164044054801, 41.33714233314145, -81.34076747300007, 70.99341851060123


def cos_turns(turns, scale):
    r = turns - jnp.round(turns)
    u = jnp.abs(r) - 0.25
    w = u * u
    poly = ((C7 * scale * w + C5 * scale) * w + C3 * scale) * w + C1 * scale
    return poly * u


def tdot(left, right, precision=None):
    return lax.dot_general(
        left, right, (((0,), (0,)), ((), ())), precision=precision, preferred_element_type=jnp.float32
    )


def row_of(x, r):
    return jnp.broadcast_to(x[r:r + 1, :], x.shape)


def lane_of(x, c):
    return jnp.broadcast_to(x[:, c:c + 1], x.shape)


def leaf(blocks, one):
    n = NB // 8
    sub = lax.broadcasted_iota(jnp.int32, (8, NB), 0)
    lane = lax.broadcasted_iota(jnp.int32, (8, NB), 1)
    a = list(blocks)
    e = [jnp.where(lane == sub + 8 * m, 1.0, 0.0).astype(jnp.float32) for m in range(n)]

    def cols(m, k):
        return [lane_of(a[m], 8 * k + c) for c in range(8)]

    outs = []
    v, n1 = [x * one for x in cols(0, 0)], [x * one for x in cols(1, 0)]
    for k in range(n):
        pa, pe = a[k], e[k]
        has1, has2 = k + 1 < n, k + 2 < n
        far = {m: cols(m, k) for m in range(k + 2, n)}
        if has1:
            vn = cols(k + 1, k + 1)
        if has2:
            n2 = list(far[k + 2])
        rs = jnp.zeros((8, NB), jnp.float32)
        dv = jnp.zeros((8, NB), jnp.float32)
        for r in range(8):
            d = row_of(v[r], r)
            inv = 1.0 / d
            rs = jnp.where(sub == r, lax.rsqrt(d), rs)
            dv = jnp.where(sub == r, inv, dv)
            l = jnp.where(sub > r, v[r] * inv, 0.0)
            b = {c: row_of(v[c], r) for c in range(r + 1, 8)}
            ba, be = row_of(pa, r), row_of(pe, r)
            for c in b:
                v[c] = v[c] - l * b[c]
            pa = pa - l * ba
            pe = pe - l * be
            if has1:
                l1 = n1[r] * inv
                w = [row_of(n1[r], c) for c in range(8)]
                for c in b:
                    n1[c] = n1[c] - l1 * b[c]
                for c in range(8):
                    vn[c] = vn[c] - l1 * w[c]
                a[k + 1] = a[k + 1] - l1 * ba
                e[k + 1] = e[k + 1] - l1 * be
            if has2:
                l2 = n2[r] * inv
                for c in b:
                    n2[c] = n2[c] - l2 * b[c]
                a[k + 2] = a[k + 2] - l2 * ba
                e[k + 2] = e[k + 2] - l2 * be
        outs.append((pa * rs, pe * rs))
        if k + 3 < n:
            qa, qe = pa * dv, pe * dv
            for r in range(7, 0, -1):
                mult = jnp.where(sub < r, v[r] * dv, 0.0)
                qa = qa - mult * row_of(qa, r)
                qe = qe - mult * row_of(qe, r)
            ra = [row_of(qa, r) for r in range(8)]
            re = [row_of(qe, r) for r in range(8)]
            for m in range(k + 3, n):
                ma = [far[m][r] * ra[r] for r in range(8)]
                me = [far[m][r] * re[r] for r in range(8)]
                while len(ma) > 1:
                    ma = [ma[i] + ma[i + 1] for i in range(0, len(ma), 2)]
                    me = [me[i] + me[i + 1] for i in range(0, len(me), 2)]
                a[m] = a[m] - ma[0]
                e[m] = e[m] - me[0]
        if has1:
            v = vn
            if has2:
                n1 = [x * one for x in cols(k + 2, k + 1)]
    return outs


def fused(scale, points_in, targets_in, freqs_in, phase_in, ridge_in, slab, gram, proj,
          points, pack, freqs, small, other_f, other_s, tile_f, tile_s, wphi, cphi, tgt, slab_in, gram_out, gram_in, proj_part, proj_in,
          up_send, up_recv, dn_send, dn_recv, pair_send, pair_recv, tree_recv, row_send, col_send,
          tile_send, tile_recv, swap_send, swap_recv, local_sem, load_sem):
    data, feat = lax.axis_index("dp"), lax.axis_index("feat")
    z, core = data // 2, data % 2
    x, y = feat // YS, feat % YS
    block, half = 256, freqs.shape[1]
    loads = [
        pltpu.make_async_copy(points_in, pack.at[pl.ds(0, block)], load_sem.at[0]),
        pltpu.make_async_copy(targets_in, pack.at[pl.ds(block, 8)], load_sem.at[1]),
        pltpu.make_async_copy(freqs_in, freqs, load_sem.at[2]),
        pltpu.make_async_copy(phase_in, small.at[pl.ds(0, 1)], load_sem.at[3]),
        pltpu.make_async_copy(ridge_in, small.at[pl.ds(1, 1)], load_sem.at[4]),
    ]
    for load in loads:
        load.start()
    odd = feat % 2
    own = pl.multiple_of(odd * half, half)
    oth = pl.multiple_of((1 - odd) * half, half)

    def at(zz, cc):
        return {"dp": zz * 2 + cc, "feat": feat}

    def near(xx, yy):
        return {"dp": data, "feat": xx * YS + yy}

    up, dn, mate = at((z + 1) % ZS, core), at((z + ZS - 1) % ZS, core), at(z, 1 - core)
    barrier = pltpu.get_barrier_semaphore()
    peers = [up, dn, mate]
    peers += [near((x + i) % XS, y) for i in range(1, XS)] + [near(x, (y + i) % YS) for i in range(1, YS)]
    for peer in peers:
        pl.semaphore_signal(barrier, inc=1, device_id=peer, device_id_type=MESH)
    for load in loads:
        load.wait()
    pl.semaphore_wait(barrier, len(peers))

    count = up_send.shape[1]
    cuts = [i * (block // count) for i in range(count)] + [pack.shape[0]]
    pieces = [pl.ds(lo, hi - lo) for lo, hi in zip(cuts[:-1], cuts[1:])]
    sends = []

    def remote(src, dst, ssem, rsem, where):
        return pltpu.make_async_remote_copy(
            src_ref=src, dst_ref=dst, send_sem=ssem, recv_sem=rsem, device_id=where, device_id_type=MESH)

    def go(copy):
        copy.start()
        sends.append(copy)
        return copy

    def arrival(step, upward):
        return 7 if step == 4 else 2 * step - (1 if upward else 0)

    def ring(step, p, upward):
        src = pack if step == 0 else points.at[arrival(step, upward)]
        dst = points.at[arrival(step + 1, upward)]
        ssem, rsem, where = (up_send, up_recv, up) if upward else (dn_send, dn_recv, dn)
        return remote(src.at[pieces[p]], dst.at[pieces[p]], ssem.at[step, p], rsem.at[step, p], where)

    def ring_step(step):
        for p in range(count):
            for upward in (True, False):
                mine = (p < count // 2) == upward
                if step == 4 and not mine:
                    continue
                ring(step - 1, p, upward).wait_recv()
                if step < 3 or (step == 3 and mine):
                    go(ring(step, p, upward))

    for p in range(count):
        go(ring(0, p, True))
        go(ring(0, p, False))
    pair = near(x, y + 1 - 2 * (y % 2))
    part_rows = freqs.shape[0] // 2
    here = pl.ds(pl.multiple_of(core * part_rows, part_rows), part_rows)
    pair_copies = [
        go(remote(small, other_s, pair_send.at[0], pair_recv.at[0], pair)),
        go(remote(freqs.at[here], other_f.at[here], pair_send.at[1], pair_recv.at[1], pair)),
    ]

    def pair_ready():
        for copy in pair_copies:
            copy.wait_recv()
        return go(remote(other_f.at[here], other_f.at[here], pair_send.at[2], pair_recv.at[2], mate))

    rx, ry = data // YS, data % YS
    parts = [(small, tile_s.at[0], None), (freqs, tile_f.at[0], pl.ds(0, 128)), (freqs, tile_f.at[0], pl.ds(128, 128))]

    def part(ref, cut):
        return ref if cut is None else ref.at[cut]

    def to_row(n, i):
        src, dst, cut = parts[n]
        return remote(part(src, cut), part(dst, cut), row_send.at[n, i], tree_recv.at[n], near((x + i + 1) % XS, y))

    def to_col(n, i, mine):
        src, dst, cut = parts[n]
        return remote(part(src if mine else dst, cut), part(dst, cut), col_send.at[n, i], tree_recv.at[n],
                      near(x, (y + i + 1) % YS))

    root = jnp.logical_and(x == rx, y == ry)
    mid = jnp.logical_and(x != rx, y == ry)

    @pl.when(root)
    def _():
        for n in range(3):
            for i in range(XS - 1):
                to_row(n, i).start()
            for i in range(YS - 1):
                to_col(n, i, True).start()
        a = pltpu.make_async_copy(freqs, tile_f.at[0], local_sem.at[0])
        b = pltpu.make_async_copy(small, tile_s.at[0], local_sem.at[1])
        a.start()
        b.start()
        a.wait()
        b.wait()

    def pass_on(n):
        @pl.when(mid)
        def _():
            to_row(n, 0).wait_recv()
            for i in range(YS - 1):
                to_col(n, i, False).start()

    def phi(i, src, sm, dst, base):
        block_ref = pack if i == 0 else points.at[i]

        for j in range(0, half, 256):
            ang = jnp.dot(block_ref[0:block, :], src[:, j:j + 256], preferred_element_type=jnp.float32)
            to = pl.ds(pl.multiple_of(base + j, 256), 256)
            dst[i * block:(i + 1) * block, to] = cos_turns(
                ang * TURN + sm[0:1, j:j + 256] * TURN, scale).astype(jnp.bfloat16)

    def mine(i):
        phi(i, freqs, small, wphi, own)
        block_ref = pack if i == 0 else points.at[i]
        tgt[:, i * block:(i + 1) * block] = block_ref[block:block + 8, :]

    def others(i):
        phi(i, other_f, other_s, wphi, oth)

    def tiles(i):
        for j in range(2):
            phi(i, tile_f.at[j], tile_s.at[j], cphi, j * half)

    def swap(n):
        cut = (pl.ds(n * 256, 256), pl.ds(n * 256, FB - n * 256))
        return remote(slab.at[cut], slab_in.at[cut], swap_send.at[n], swap_recv.at[n], mate)

    mine(0)
    ring_step(1)
    mine(1)
    mine(2)
    pass_on(0)
    pass_on(1)
    ring_step(2)
    pass_on(2)
    from_mate = pair_ready()
    mine(3)
    mine(4)
    from_mate.wait_recv()
    for i in range(3):
        others(i)
    ring_step(3)
    for i in (3, 4):
        others(i)
    for i in (5, 6):
        mine(i)
        others(i)

    @pl.when(y != ry)
    def _():
        for n in range(3):
            to_col(n, 0, False).wait_recv()

    tile_copies = [
        go(remote(tile_s.at[0], tile_s.at[1], tile_send.at[0], tile_recv.at[0], mate)),
        go(remote(tile_f.at[0], tile_f.at[1], tile_send.at[1], tile_recv.at[1], mate)),
    ]
    k0 = 6 * block
    for i in range(0, FB, 256):
        slab[i:i + 256, i:] = tdot(wphi[0:k0, i:i + 256], wphi[0:k0, i:])
    for copy in tile_copies:
        copy.wait_recv()
    for i in range(2):
        tiles(i)
    ring_step(4)
    mine(7)
    others(7)
    for n in range(4):
        i = n * 256
        slab[i:i + 256, i:] += tdot(wphi[k0:, i:i + 256], wphi[k0:, i:])
        if n > 0:
            swap(n - 1).start()
    own_cut = pl.ds(own, half)
    proj_part[...] = jnp.dot(tgt[...], wphi[:, own_cut], preferred_element_type=jnp.float32)
    swap(3).start()
    for i in range(2, 8):
        phi(i, tile_f.at[1], tile_s.at[1], cphi, half)
    proj_copy = go(remote(proj_part, proj_in, swap_send.at[5], swap_recv.at[5], mate))
    gram_out[...] = tdot(wphi[:, own_cut], cphi[:, half:])
    for i in range(2, 8):
        phi(i, tile_f.at[0], tile_s.at[0], cphi, 0)
    gram_copy = go(remote(gram_out, gram_in, swap_send.at[4], swap_recv.at[4], mate))
    gram[...] = tdot(wphi[:, own_cut], cphi[:, 0:half])

    eye = lax.broadcasted_iota(jnp.int32, (NB, NB), 0) == lax.broadcasted_iota(jnp.int32, (NB, NB), 1)
    for n in range(4):
        swap(n).wait_send()
        swap(n).wait_recv()
        i = n * 256
        slab[i:i + 256, i:] += slab_in[i:i + 256, i:]
    for sm, base in ((small, own), (other_s, oth)):
        for i in range(0, half, NB):
            to = pl.ds(pl.multiple_of(base + i, NB), NB)
            slab[to, to] += jnp.where(eye, sm[1:2, i:i + NB], 0.0)
    gram_copy.wait_recv()
    gram[...] += gram_in[...]

    @pl.when(feat == data)
    def _():
        for i in range(0, half, NB):
            gram[i:i + NB, i:i + NB] += jnp.where(eye, small[1:2, i:i + NB], 0.0)

    proj_copy.wait_recv()
    proj[...] = proj_part[...] + proj_in[...]

    @pl.when(root)
    def _():
        for n in range(3):
            for i in range(XS - 1):
                to_row(n, i).wait_send()

    @pl.when(y == ry)
    def _():
        for n in range(3):
            for i in range(YS - 1):
                to_col(n, i, False).wait_send()

    for copy in sends:
        copy.wait_send()


def assemble(scale, points, targets, freqs, phase, ridge):
    dma = pltpu.SemaphoreType.DMA
    vmem = pl.BlockSpec(memory_space=pltpu.VMEM)
    hold = pl.BlockSpec(memory_space=pl.ANY)
    f32, bf16 = jnp.float32, jnp.bfloat16
    half = freqs.shape[1]
    shape = jax.ShapeDtypeStruct
    rows = ZS * 256
    pack, small = (points.shape[0] + targets.shape[0], points.shape[1]), (2, half)
    return pl.pallas_call(
        functools.partial(fused, scale),
        out_shape=(shape((FB, FB), f32), shape((half, half), f32), shape((8, half), f32)),
        in_specs=[hold] * 5,
        out_specs=(vmem,) * 3,
        scratch_shapes=[
            pltpu.VMEM((ZS,) + pack, bf16), pltpu.VMEM(pack, bf16), pltpu.VMEM(freqs.shape, bf16), pltpu.VMEM(small, f32),
            pltpu.VMEM(freqs.shape, bf16), pltpu.VMEM(small, f32),
            pltpu.VMEM((2,) + freqs.shape, bf16), pltpu.VMEM((2,) + small, f32),
            pltpu.VMEM((rows, FB), bf16), pltpu.VMEM((rows, 2 * half), bf16), pltpu.VMEM((8, rows), bf16),
            pltpu.VMEM((FB, FB), f32), pltpu.VMEM((half, half), f32), pltpu.VMEM((half, half), f32),
            pltpu.VMEM((8, half), f32), pltpu.VMEM((8, half), f32),
            dma((4, PIECES)), dma((4, PIECES)), dma((4, PIECES)), dma((4, PIECES)),
            dma((3,)), dma((3,)), dma((3,)), dma((3, 3)), dma((3, 3)),
            dma((2,)), dma((2,)), dma((6,)), dma((6,)), dma((2,)), dma((5,)),
        ],
        compiler_params=pltpu.CompilerParams(
            collective_id=0, has_side_effects=True, vmem_limit_bytes=32 * 1024 * 1024),
    )(points, targets, freqs, phase, ridge)


def three(x):
    hi = x.astype(jnp.bfloat16)
    rest = x - hi.astype(jnp.float32)
    mid = rest.astype(jnp.bfloat16)
    return hi, mid, (rest - mid.astype(jnp.float32)).astype(jnp.bfloat16)


def left_terms(x):
    h, m, l = three(x)
    return jnp.concatenate([h, h, m, h, l, m], axis=1)


def right_terms(x):
    h, m, l = three(x)
    return jnp.concatenate([h, m, h, l, h, m], axis=0)


def chol(feat_axis, src, gram_src, proj_src, fac, slab, gram, proj, facv, ue, ones, sem):
    half = facv.shape[0]
    odd = lax.rem(lax.axis_index(feat_axis), FB // half)
    own = pl.multiple_of(odd * half, half)
    nblk = FB // NB
    through = [pltpu.make_async_copy(gram_src, gram, sem.at[nblk]), pltpu.make_async_copy(proj_src, proj, sem.at[nblk + 1])]
    for copy in through:
        copy.start()
    ones[...] = jnp.ones_like(ones)

    def column(k):
        cut = pl.ds(pl.multiple_of(k * NB, NB), NB)
        return pltpu.make_async_copy(facv.at[:, cut], fac.at[:, cut], sem.at[k])

    def step(k, _):
        at = pl.multiple_of(k * NB, NB)
        blocks = [slab[pl.ds(pl.multiple_of(at + 8 * m, 8), 8), pl.ds(at, NB)] for m in range(NB // 8)]
        sub = lax.broadcasted_iota(jnp.int32, (8, NB), 0)
        lane = lax.broadcasted_iota(jnp.int32, (8, NB), 1)
        for m, (u, x) in enumerate(leaf(blocks, ones[...])):
            slab[pl.ds(pl.multiple_of(at + 8 * m, 8), 8), pl.ds(at, NB)] = jnp.where(lane >= sub + 8 * m, u, 0.0)
            ue[8 * m:8 * m + 8, :] = x
        for kk in range(nblk - 1):
            @pl.when(k == kk)
            def _():
                lo, mid = kk * NB, (kk + 1) * NB
                u12 = jnp.dot(left_terms(ue[...]), right_terms(slab[lo:mid, mid:]), preferred_element_type=jnp.float32)
                slab[lo:mid, mid:] = u12
                left, right = left_terms(jnp.transpose(u12)), right_terms(u12)
                for i in range(0, FB - mid, 256):
                    w = min(256, FB - mid - i)
                    slab[mid + i:mid + i + w, mid + i:] -= jnp.dot(
                        left[i:i + w], right[:, i:], preferred_element_type=jnp.float32)
        for b in range(half // NB):
            piece = jnp.transpose(slab[pl.ds(at, NB), pl.ds(pl.multiple_of(own + b * NB, NB), NB)])
            facv[b * NB:(b + 1) * NB, pl.ds(at, NB)] = jnp.where(at <= own + b * NB, piece, 0.0)
        column(k).start()
        return 0

    lax.fori_loop(0, nblk, step, 0)
    for k in range(nblk):
        column(k).wait()
    for copy in through:
        copy.wait()


def factor(slab, gram, proj, flags=None):
    f32 = jnp.float32
    hold = pl.BlockSpec(memory_space=pl.ANY)
    vmem = pl.BlockSpec(memory_space=pltpu.VMEM)
    shape = jax.ShapeDtypeStruct
    fac, _, gram, proj = pl.pallas_call(
        functools.partial(chol, "feat"),
        out_shape=(shape((FB // 2, FB), f32), shape(slab.shape, f32), shape(gram.shape, f32), shape(proj.shape, f32)),
        in_specs=[vmem, hold, hold],
        out_specs=(hold, vmem, hold, hold),
        input_output_aliases={0: 1},
        scratch_shapes=[
            pltpu.VMEM((FB // 2, FB), f32),
            pltpu.VMEM((NB, NB), f32),
            pltpu.VMEM((8, NB), f32),
            pltpu.SemaphoreType.DMA((FB // NB + 2,)),
        ],
        compiler_params=pltpu.CompilerParams(vmem_limit_bytes=20 * 1024 * 1024, flags=flags),
    )(slab, gram, proj)
    return gram, proj, fac


def shards(points, freqs, phase, ridge, targets):
    scale = math.sqrt(2.0 / (points.shape[0] * lax.axis_size("dp")))
    stay = [pltpu.with_memory_space_constraint(v, pltpu.HBM) for v in (points, targets, freqs, phase[None], ridge[None])]
    slab, gram, proj = assemble(scale, *stay)
    return factor(slab, gram, proj)


def solution(mesh):
    in_specs = (P("dp", None), P(None, "feat"), P("feat"), P("feat"), P(None, "dp"))
    out_specs = (P("feat", "dp"), P(None, "feat"), P("feat", None))
    return jax.shard_map(shards, mesh=mesh, in_specs=in_specs, out_specs=out_specs, check_vma=False)
```

```python
import functools
import math

import jax
import jax.numpy as jnp
from jax import lax
from jax.experimental import pallas as pl
from jax.experimental.pallas import tpu as pltpu
from jax.sharding import PartitionSpec as P

FB = 1024
NB = 128
XS = 4
YS = 4
ZS = 8
PIECES = 4
HI = lax.Precision.HIGHEST
MESH = pl.DeviceIdType.MESH
TURN = 1.0 / (2.0 * math.pi)
C1, C3, C5, C7 = -6.283164044054801, 41.33714233314145, -81.34076747300007, 70.99341851060123


def cos_turns(turns, scale):
    r = turns - jnp.round(turns)
    u = jnp.abs(r) - 0.25
    w = u * u
    poly = ((C7 * scale * w + C5 * scale) * w + C3 * scale) * w + C1 * scale
    return poly * u


def tdot(left, right, precision=None):
    return lax.dot_general(
        left, right, (((0,), (0,)), ((), ())), precision=precision, preferred_element_type=jnp.float32
    )


def row_of(x, r):
    return jnp.broadcast_to(x[r:r + 1, :], x.shape)


def lane_of(x, c):
    return jnp.broadcast_to(x[:, c:c + 1], x.shape)


def leaf(blocks, one):
    n = NB // 8
    sub = lax.broadcasted_iota(jnp.int32, (8, NB), 0)
    lane = lax.broadcasted_iota(jnp.int32, (8, NB), 1)
    a = list(blocks)
    e = [jnp.where(lane == sub + 8 * m, 1.0, 0.0).astype(jnp.float32) for m in range(n)]

    def cols(m, k):
        return [lane_of(a[m], 8 * k + c) for c in range(8)]

    outs = []
    v, n1 = [x * one for x in cols(0, 0)], [x * one for x in cols(1, 0)]
    for k in range(n):
        pa, pe = a[k], e[k]
        has1, has2 = k + 1 < n, k + 2 < n
        far = {m: cols(m, k) for m in range(k + 2, n)}
        if has1:
            vn = cols(k + 1, k + 1)
        if has2:
            n2 = list(far[k + 2])
        rs = jnp.zeros((8, NB), jnp.float32)
        dv = jnp.zeros((8, NB), jnp.float32)
        for r in range(8):
            d = row_of(v[r], r)
            inv = 1.0 / d
            rs = jnp.where(sub == r, lax.rsqrt(d), rs)
            dv = jnp.where(sub == r, inv, dv)
            l = jnp.where(sub > r, v[r] * inv, 0.0)
            b = {c: row_of(v[c], r) for c in range(r + 1, 8)}
            ba, be = row_of(pa, r), row_of(pe, r)
            for c in b:
                v[c] = v[c] - l * b[c]
            pa = pa - l * ba
            pe = pe - l * be
            if has1:
                l1 = n1[r] * inv
                w = [row_of(n1[r], c) for c in range(8)]
                for c in b:
                    n1[c] = n1[c] - l1 * b[c]
                for c in range(8):
                    vn[c] = vn[c] - l1 * w[c]
                a[k + 1] = a[k + 1] - l1 * ba
                e[k + 1] = e[k + 1] - l1 * be
            if has2:
                l2 = n2[r] * inv
                for c in b:
                    n2[c] = n2[c] - l2 * b[c]
                a[k + 2] = a[k + 2] - l2 * ba
                e[k + 2] = e[k + 2] - l2 * be
        outs.append((pa * rs, pe * rs))
        if k + 3 < n:
            qa, qe = pa * dv, pe * dv
            for r in range(7, 0, -1):
                mult = jnp.where(sub < r, v[r] * dv, 0.0)
                qa = qa - mult * row_of(qa, r)
                qe = qe - mult * row_of(qe, r)
            ra = [row_of(qa, r) for r in range(8)]
            re = [row_of(qe, r) for r in range(8)]
            for m in range(k + 3, n):
                ma = [far[m][r] * ra[r] for r in range(8)]
                me = [far[m][r] * re[r] for r in range(8)]
                while len(ma) > 1:
                    ma = [ma[i] + ma[i + 1] for i in range(0, len(ma), 2)]
                    me = [me[i] + me[i + 1] for i in range(0, len(me), 2)]
                a[m] = a[m] - ma[0]
                e[m] = e[m] - me[0]
        if has1:
            v = vn
            if has2:
                n1 = [x * one for x in cols(k + 2, k + 1)]
    return outs


def fused(scale, points_in, targets_in, freqs_in, phase_in, ridge_in, slab, gram, proj,
          points, pack, freqs, small, other_f, other_s, tile_f, tile_s, wphi, cphi, tgt, slab_in, gram_out, gram_in, proj_part, proj_in,
          up_send, up_recv, dn_send, dn_recv, pair_send, pair_recv, tree_recv, row_send, col_send,
          tile_send, tile_recv, swap_send, swap_recv, local_sem, load_sem):
    data, feat = lax.axis_index("dp"), lax.axis_index("feat")
    z, core = data // 2, data % 2
    x, y = feat // YS, feat % YS
    block, half = 256, freqs.shape[1]
    loads = [
        pltpu.make_async_copy(points_in, pack.at[pl.ds(0, block)], load_sem.at[0]),
        pltpu.make_async_copy(targets_in, pack.at[pl.ds(block, 8)], load_sem.at[1]),
        pltpu.make_async_copy(freqs_in, freqs, load_sem.at[2]),
        pltpu.make_async_copy(phase_in, small.at[pl.ds(0, 1)], load_sem.at[3]),
        pltpu.make_async_copy(ridge_in, small.at[pl.ds(1, 1)], load_sem.at[4]),
    ]
    for load in loads:
        load.start()
    odd = feat % 2
    own = pl.multiple_of(odd * half, half)
    oth = pl.multiple_of((1 - odd) * half, half)

    def at(zz, cc):
        return {"dp": zz * 2 + cc, "feat": feat}

    def near(xx, yy):
        return {"dp": data, "feat": xx * YS + yy}

    up, dn, mate = at((z + 1) % ZS, core), at((z + ZS - 1) % ZS, core), at(z, 1 - core)
    barrier = pltpu.get_barrier_semaphore()
    peers = [up, dn, mate]
    peers += [near((x + i) % XS, y) for i in range(1, XS)] + [near(x, (y + i) % YS) for i in range(1, YS)]
    for peer in peers:
        pl.semaphore_signal(barrier, inc=1, device_id=peer, device_id_type=MESH)
    for load in loads:
        load.wait()
    pl.semaphore_wait(barrier, len(peers))

    count = up_send.shape[1]
    cuts = [i * (block // count) for i in range(count)] + [pack.shape[0]]
    pieces = [pl.ds(lo, hi - lo) for lo, hi in zip(cuts[:-1], cuts[1:])]
    sends = []

    def remote(src, dst, ssem, rsem, where):
        return pltpu.make_async_remote_copy(
            src_ref=src, dst_ref=dst, send_sem=ssem, recv_sem=rsem, device_id=where, device_id_type=MESH)

    def go(copy):
        copy.start()
        sends.append(copy)
        return copy

    def arrival(step, upward):
        return 7 if step == 4 else 2 * step - (1 if upward else 0)

    def ring(step, p, upward):
        src = pack if step == 0 else points.at[arrival(step, upward)]
        dst = points.at[arrival(step + 1, upward)]
        ssem, rsem, where = (up_send, up_recv, up) if upward else (dn_send, dn_recv, dn)
        return remote(src.at[pieces[p]], dst.at[pieces[p]], ssem.at[step, p], rsem.at[step, p], where)

    def ring_step(step):
        for p in range(count):
            for upward in (True, False):
                mine = (p < count // 2) == upward
                if step == 4 and not mine:
                    continue
                ring(step - 1, p, upward).wait_recv()
                if step < 3 or (step == 3 and mine):
                    go(ring(step, p, upward))

    for p in range(count):
        go(ring(0, p, True))
        go(ring(0, p, False))
    pair = near(x, y + 1 - 2 * (y % 2))
    part_rows = freqs.shape[0] // 2
    here = pl.ds(pl.multiple_of(core * part_rows, part_rows), part_rows)
    pair_copies = [
        go(remote(small, other_s, pair_send.at[0], pair_recv.at[0], pair)),
        go(remote(freqs.at[here], other_f.at[here], pair_send.at[1], pair_recv.at[1], pair)),
    ]

    def pair_ready():
        for copy in pair_copies:
            copy.wait_recv()
        return go(remote(other_f.at[here], other_f.at[here], pair_send.at[2], pair_recv.at[2], mate))

    rx, ry = data // YS, data % YS
    parts = [(small, tile_s.at[0], None), (freqs, tile_f.at[0], pl.ds(0, 128)), (freqs, tile_f.at[0], pl.ds(128, 128))]

    def part(ref, cut):
        return ref if cut is None else ref.at[cut]

    def to_row(n, i):
        src, dst, cut = parts[n]
        return remote(part(src, cut), part(dst, cut), row_send.at[n, i], tree_recv.at[n], near((x + i + 1) % XS, y))

    def to_col(n, i, mine):
        src, dst, cut = parts[n]
        return remote(part(src if mine else dst, cut), part(dst, cut), col_send.at[n, i], tree_recv.at[n],
                      near(x, (y + i + 1) % YS))

    root = jnp.logical_and(x == rx, y == ry)
    mid = jnp.logical_and(x != rx, y == ry)

    @pl.when(root)
    def _():
        for n in range(3):
            for i in range(XS - 1):
                to_row(n, i).start()
            for i in range(YS - 1):
                to_col(n, i, True).start()
        a = pltpu.make_async_copy(freqs, tile_f.at[0], local_sem.at[0])
        b = pltpu.make_async_copy(small, tile_s.at[0], local_sem.at[1])
        a.start()
        b.start()
        a.wait()
        b.wait()

    def pass_on(n):
        @pl.when(mid)
        def _():
            to_row(n, 0).wait_recv()
            for i in range(YS - 1):
                to_col(n, i, False).start()

    def phi(i, src, sm, dst, base):
        block_ref = pack if i == 0 else points.at[i]

        for j in range(0, half, 256):
            ang = jnp.dot(block_ref[0:block, :], src[:, j:j + 256], preferred_element_type=jnp.float32)
            to = pl.ds(pl.multiple_of(base + j, 256), 256)
            dst[i * block:(i + 1) * block, to] = cos_turns(
                ang * TURN + sm[0:1, j:j + 256] * TURN, scale).astype(jnp.bfloat16)

    def mine(i):
        phi(i, freqs, small, wphi, own)
        block_ref = pack if i == 0 else points.at[i]
        tgt[:, i * block:(i + 1) * block] = block_ref[block:block + 8, :]

    def others(i):
        phi(i, other_f, other_s, wphi, oth)

    def tiles(i):
        for j in range(2):
            phi(i, tile_f.at[j], tile_s.at[j], cphi, j * half)

    def swap(n):
        cut = (pl.ds(n * 256, 256), pl.ds(n * 256, FB - n * 256))
        return remote(slab.at[cut], slab_in.at[cut], swap_send.at[n], swap_recv.at[n], mate)

    mine(0)
    ring_step(1)
    mine(1)
    mine(2)
    pass_on(0)
    pass_on(1)
    ring_step(2)
    pass_on(2)
    from_mate = pair_ready()
    mine(3)
    mine(4)
    from_mate.wait_recv()
    for i in range(3):
        others(i)
    ring_step(3)
    for i in (3, 4):
        others(i)
    for i in (5, 6):
        mine(i)
        others(i)

    k0 = 6 * block
    for i in range(0, FB, 256):
        slab[i:i + 256, i:] = tdot(wphi[0:k0, i:i + 256], wphi[0:k0, i:])
    ring_step(4)
    @pl.when(y != ry)
    def _():
        for n in range(3):
            to_col(n, 0, False).wait_recv()

    tile_copies = [
        go(remote(tile_s.at[0], tile_s.at[1], tile_send.at[0], tile_recv.at[0], mate)),
        go(remote(tile_f.at[0], tile_f.at[1], tile_send.at[1], tile_recv.at[1], mate)),
    ]
    mine(7)
    others(7)
    for n in range(4):
        i = n * 256
        slab[i:i + 256, i:] += tdot(wphi[k0:, i:i + 256], wphi[k0:, i:])
        if n > 0:
            swap(n - 1).start()
    own_cut = pl.ds(own, half)
    proj_part[...] = jnp.dot(tgt[...], wphi[:, own_cut], preferred_element_type=jnp.float32)
    swap(3).start()
    for copy in tile_copies:
        copy.wait_recv()
    for i in range(8):
        phi(i, tile_f.at[1], tile_s.at[1], cphi, half)
    proj_copy = go(remote(proj_part, proj_in, swap_send.at[5], swap_recv.at[5], mate))
    gram_out[...] = tdot(wphi[:, own_cut], cphi[:, half:])
    for i in range(0, 8):
        phi(i, tile_f.at[0], tile_s.at[0], cphi, 0)
    gram_copy = go(remote(gram_out, gram_in, swap_send.at[4], swap_recv.at[4], mate))
    gram[...] = tdot(wphi[:, own_cut], cphi[:, 0:half])

    eye = lax.broadcasted_iota(jnp.int32, (NB, NB), 0) == lax.broadcasted_iota(jnp.int32, (NB, NB), 1)
    for n in range(4):
        swap(n).wait_send()
        swap(n).wait_recv()
        i = n * 256
        slab[i:i + 256, i:] += slab_in[i:i + 256, i:]
    for sm, base in ((small, own), (other_s, oth)):
        for i in range(0, half, NB):
            to = pl.ds(pl.multiple_of(base + i, NB), NB)
            slab[to, to] += jnp.where(eye, sm[1:2, i:i + NB], 0.0)
    gram_copy.wait_recv()
    gram[...] += gram_in[...]

    @pl.when(feat == data)
    def _():
        for i in range(0, half, NB):
            gram[i:i + NB, i:i + NB] += jnp.where(eye, small[1:2, i:i + NB], 0.0)

    proj_copy.wait_recv()
    proj[...] = proj_part[...] + proj_in[...]

    @pl.when(root)
    def _():
        for n in range(3):
            for i in range(XS - 1):
                to_row(n, i).wait_send()

    @pl.when(y == ry)
    def _():
        for n in range(3):
            for i in range(YS - 1):
                to_col(n, i, False).wait_send()

    for copy in sends:
        copy.wait_send()


def assemble(scale, points, targets, freqs, phase, ridge):
    dma = pltpu.SemaphoreType.DMA
    vmem = pl.BlockSpec(memory_space=pltpu.VMEM)
    hold = pl.BlockSpec(memory_space=pl.ANY)
    f32, bf16 = jnp.float32, jnp.bfloat16
    half = freqs.shape[1]
    shape = jax.ShapeDtypeStruct
    rows = ZS * 256
    pack, small = (points.shape[0] + targets.shape[0], points.shape[1]), (2, half)
    return pl.pallas_call(
        functools.partial(fused, scale),
        out_shape=(shape((FB, FB), f32), shape((half, half), f32), shape((8, half), f32)),
        in_specs=[hold] * 5,
        out_specs=(vmem,) * 3,
        scratch_shapes=[
            pltpu.VMEM((ZS,) + pack, bf16), pltpu.VMEM(pack, bf16), pltpu.VMEM(freqs.shape, bf16), pltpu.VMEM(small, f32),
            pltpu.VMEM(freqs.shape, bf16), pltpu.VMEM(small, f32),
            pltpu.VMEM((2,) + freqs.shape, bf16), pltpu.VMEM((2,) + small, f32),
            pltpu.VMEM((rows, FB), bf16), pltpu.VMEM((rows, 2 * half), bf16), pltpu.VMEM((8, rows), bf16),
            pltpu.VMEM((FB, FB), f32), pltpu.VMEM((half, half), f32), pltpu.VMEM((half, half), f32),
            pltpu.VMEM((8, half), f32), pltpu.VMEM((8, half), f32),
            dma((4, PIECES)), dma((4, PIECES)), dma((4, PIECES)), dma((4, PIECES)),
            dma((3,)), dma((3,)), dma((3,)), dma((3, 3)), dma((3, 3)),
            dma((2,)), dma((2,)), dma((6,)), dma((6,)), dma((2,)), dma((5,)),
        ],
        compiler_params=pltpu.CompilerParams(
            collective_id=0, has_side_effects=True, vmem_limit_bytes=32 * 1024 * 1024),
    )(points, targets, freqs, phase, ridge)


def three(x):
    hi = x.astype(jnp.bfloat16)
    rest = x - hi.astype(jnp.float32)
    mid = rest.astype(jnp.bfloat16)
    return hi, mid, (rest - mid.astype(jnp.float32)).astype(jnp.bfloat16)


def left_terms(x):
    h, m, l = three(x)
    return jnp.concatenate([h, h, m, h, l, m], axis=1)


def right_terms(x):
    h, m, l = three(x)
    return jnp.concatenate([h, m, h, l, h, m], axis=0)


def chol(feat_axis, src, gram_src, proj_src, fac, slab, gram, proj, facv, ue, ones, sem):
    half = facv.shape[0]
    odd = lax.rem(lax.axis_index(feat_axis), FB // half)
    own = pl.multiple_of(odd * half, half)
    nblk = FB // NB
    through = [pltpu.make_async_copy(gram_src, gram, sem.at[nblk]), pltpu.make_async_copy(proj_src, proj, sem.at[nblk + 1])]
    for copy in through:
        copy.start()
    ones[...] = jnp.ones_like(ones)

    def column(k):
        cut = pl.ds(pl.multiple_of(k * NB, NB), NB)
        return pltpu.make_async_copy(facv.at[:, cut], fac.at[:, cut], sem.at[k])

    def step(k, _):
        at = pl.multiple_of(k * NB, NB)
        blocks = [slab[pl.ds(pl.multiple_of(at + 8 * m, 8), 8), pl.ds(at, NB)] for m in range(NB // 8)]
        sub = lax.broadcasted_iota(jnp.int32, (8, NB), 0)
        lane = lax.broadcasted_iota(jnp.int32, (8, NB), 1)
        for m, (u, x) in enumerate(leaf(blocks, ones[...])):
            slab[pl.ds(pl.multiple_of(at + 8 * m, 8), 8), pl.ds(at, NB)] = jnp.where(lane >= sub + 8 * m, u, 0.0)
            ue[8 * m:8 * m + 8, :] = x
        for kk in range(nblk - 1):
            @pl.when(k == kk)
            def _():
                lo, mid = kk * NB, (kk + 1) * NB
                u12 = jnp.dot(left_terms(ue[...]), right_terms(slab[lo:mid, mid:]), preferred_element_type=jnp.float32)
                slab[lo:mid, mid:] = u12
                left, right = left_terms(jnp.transpose(u12)), right_terms(u12)
                for i in range(0, FB - mid, 256):
                    w = min(256, FB - mid - i)
                    slab[mid + i:mid + i + w, mid + i:] -= jnp.dot(
                        left[i:i + w], right[:, i:], preferred_element_type=jnp.float32)
        for b in range(half // NB):
            piece = jnp.transpose(slab[pl.ds(at, NB), pl.ds(pl.multiple_of(own + b * NB, NB), NB)])
            facv[b * NB:(b + 1) * NB, pl.ds(at, NB)] = jnp.where(at <= own + b * NB, piece, 0.0)
        column(k).start()
        return 0

    lax.fori_loop(0, nblk, step, 0)
    for k in range(nblk):
        column(k).wait()
    for copy in through:
        copy.wait()


def factor(slab, gram, proj, flags=None):
    f32 = jnp.float32
    hold = pl.BlockSpec(memory_space=pl.ANY)
    vmem = pl.BlockSpec(memory_space=pltpu.VMEM)
    shape = jax.ShapeDtypeStruct
    fac, _, gram, proj = pl.pallas_call(
        functools.partial(chol, "feat"),
        out_shape=(shape((FB // 2, FB), f32), shape(slab.shape, f32), shape(gram.shape, f32), shape(proj.shape, f32)),
        in_specs=[vmem, hold, hold],
        out_specs=(hold, vmem, hold, hold),
        input_output_aliases={0: 1},
        scratch_shapes=[
            pltpu.VMEM((FB // 2, FB), f32),
            pltpu.VMEM((NB, NB), f32),
            pltpu.VMEM((8, NB), f32),
            pltpu.SemaphoreType.DMA((FB // NB + 2,)),
        ],
        compiler_params=pltpu.CompilerParams(vmem_limit_bytes=20 * 1024 * 1024, flags=flags),
    )(slab, gram, proj)
    return gram, proj, fac


def shards(points, freqs, phase, ridge, targets):
    scale = math.sqrt(2.0 / (points.shape[0] * lax.axis_size("dp")))
    stay = [pltpu.with_memory_space_constraint(v, pltpu.HBM) for v in (points, targets, freqs, phase[None], ridge[None])]
    slab, gram, proj = assemble(scale, *stay)
    return factor(slab, gram, proj)


def solution(mesh):
    in_specs = (P("dp", None), P(None, "feat"), P("feat"), P("feat"), P(None, "dp"))
    out_specs = (P("feat", "dp"), P(None, "feat"), P("feat", None))
    return jax.shard_map(shards, mesh=mesh, in_specs=in_specs, out_specs=out_specs, check_vma=False)
```
